32 devices in a mesh: gauss: 8 (over z, core), img: 4 (over y, x).
Axes of the slice: x: 2, y: 2, z: 4, core: 2. Of those that a mesh axis runs over, the one named last changes fastest.
Arguments:
- observed: bfloat16 [16, 256, 256], P('img', 'gauss'), may hold values from -6 to 6
- pose_index: int32 [16], P('img'), may hold values from 0 to 4095
- batch_order: int32 [16], P('img'), may hold values from 0 to 3, as said below
- latents: float32 [16, 16], P('img'), may hold values from -3 to 3
- base_positions: float32 [3, 65536], P(None, 'gauss'), may hold values from -70 to 69
- amplitudes: float32 [65536], P('gauss'), may hold values from -1.25 to 1.25
- widths: float32 [65536], P('gauss'), may hold values from 1 to 3
- deform_modes: float32 [16, 3, 65536], P(None, None, ('gauss', 'img')), may hold values from -12 to 12
Outputs:
- final_residual: float32 [4, 256, 256], P('img', 'gauss')
- new_modes: float32 [16, 3, 65536], P(None, None, ('gauss', 'img'))
The draws below stay inside these ranges and needn't reach their ends.
Inputs may be any that keep to these rules, and one draw needn't show every extreme that they name: `batch_order`: in each aligned block of 4 entries (one device's images) every number from 0 to 3 appears exactly once.
All inputs are finite; a program needn't handle non-finite values.
Results may differ from the reference program's by a relative error of at most 0.0045.
Values may be sent and summed in bfloat16 or wider, within the bound.
No kernel may reach another device: no remote copies, remote signals or barrier semaphores. Data moves between devices by JAX's collectives and lax.ppermute only.
A program may use at most 64 MiB of HBM per device.

```python
import math
import jax
import jax.numpy as jnp
from jax import lax

PIX = 256
K = 16
NROT = 4096
STEPS = 2
IMG_DEV = 4
G_DEV = 8192
GAUSSIANS = 65536
IMAGES = 16
BATCH = 4


def draw_batch_order(key, part):
    keys = jax.random.split(key, IMAGES // IMG_DEV)
    orders = jax.vmap(lambda one_key: jax.random.permutation(one_key, IMG_DEV))(keys)
    return orders.reshape(-1).astype(jnp.int32)


def set_ends(entries, stream_key, least, largest):
    extent = entries.shape
    place = [jax.random.randint(jax.random.fold_in(stream_key, axis), (), 0, extent[axis]) for axis in range(len(extent))]
    entries = entries.at[tuple(place)].set(least)
    longest = extent.index(max(extent))
    place[longest] = (place[longest] + 1) % extent[longest]
    return entries.at[tuple(place)].set(largest)


def levels(own_key, shape, cuts, low, largest):
    def one(axis_at, shards_of):
        draws = jax.random.uniform(jax.random.fold_in(jax.random.fold_in(own_key, 6), axis_at), (shards_of,), jnp.float32, low / len(cuts), largest / len(cuts))
        return jnp.repeat(jnp.exp(draws), shape[axis_at] // shards_of).reshape((-1,) + (1,) * (len(shape) - axis_at - 1))

    loudness = one(*cuts[0])
    for cut in cuts[1:]:
        loudness = loudness * one(*cut)
    return loudness


def scatter_about(stream_key, dims, spread, bound, cuts=(), kind=jnp.bfloat16):
    values = spread * jax.random.normal(stream_key, dims, jnp.float32)
    if cuts:
        values = values * levels(stream_key, dims, cuts, -0.22, 0.18)
    return jnp.clip(values, -bound, bound).astype(kind)


def setup_inputs(seed: int = 0) -> dict:
    key_of = jax.random.split(jax.random.key(seed), 9)
    return {
        "observed": scatter_about(key_of[0], (IMAGES, PIX, PIX), 1.0, 6.0, ((0, 4), (1, 8))),
        "pose_index": set_ends(jax.random.randint(key_of[1], (IMAGES,), 0, NROT), jax.random.fold_in(key_of[1], 1), 0, NROT - 1).astype(jnp.int32),
        "batch_order": draw_batch_order(jax.random.fold_in(key_of[8], 71), 0),
        "latents": scatter_about(key_of[3], (IMAGES, K), 0.5, 3.0, ((0, 4),), jnp.float32),
        "base_positions": jnp.clip(-70.0 + 139.0 * jax.random.uniform(key_of[4], (3, GAUSSIANS), jnp.float32) ** levels(key_of[4], (3, GAUSSIANS), ((1, 8),), -0.2, 0.2), -70.0, 69.0),
        "amplitudes": scatter_about(key_of[5], (GAUSSIANS,), (24 * GAUSSIANS // (PIX * PIX)) ** -0.5, 1.25, ((0, 8),), jnp.float32),
        "widths": jnp.clip(jnp.exp(math.log(3.0) - 1.0986123 * jax.random.uniform(key_of[6], (GAUSSIANS,), jnp.float32) ** levels(key_of[6], (GAUSSIANS,), ((0, 8),), -0.2, 0.2)), 1.0, 3.0),
        "deform_modes": scatter_about(key_of[7], (K, 3, GAUSSIANS), 2.0, 12.0, ((2, 32),), jnp.float32),
    }


step_size = 0.5
tiny_eps = 1e-06

def rotation_rows(pose_id):
    cos_beta = 1.0 - (2 * pose_id + 1).astype(jnp.float32) / NROT
    sin_beta = jnp.sqrt(1.0 - cos_beta * cos_beta)
    alpha = (pose_id * 55 % 144).astype(jnp.float32) * (2.0 * math.pi / 144.0)
    gamma = (pose_id % 8).astype(jnp.float32) * (math.pi / 4.0)
    cos_alpha, sin_alpha = (jnp.cos(alpha), jnp.sin(alpha))
    cos_gamma, sin_gamma = (jnp.cos(gamma), jnp.sin(gamma))
    first = jnp.stack([cos_alpha * cos_beta * cos_gamma - sin_alpha * sin_gamma, -cos_alpha * cos_beta * sin_gamma - sin_alpha * cos_gamma, cos_alpha * sin_beta])
    second = jnp.stack([sin_alpha * cos_beta * cos_gamma + cos_alpha * sin_gamma, -sin_alpha * cos_beta * sin_gamma + cos_alpha * cos_gamma, sin_alpha * sin_beta])
    return jnp.stack([first, second])

def factors(positions, rotation, amplitudes, widths):
    center = (PIX - 1) * 0.5
    proj_u = rotation[0, 0] * positions[0] + rotation[0, 1] * positions[1] + rotation[0, 2] * positions[2] + center
    proj_v = rotation[1, 0] * positions[0] + rotation[1, 1] * positions[1] + rotation[1, 2] * positions[2] + center
    pixels = jnp.arange(PIX).astype(jnp.float32)
    inv_var = 1.0 / (widths * widths)
    diff_u = pixels[None, :] - proj_u[:, None]
    diff_v = pixels[None, :] - proj_v[:, None]
    profile_u = jnp.exp(-0.5 * diff_u * diff_u * inv_var[:, None]).astype(jnp.bfloat16)
    profile_v = (amplitudes[:, None] * jnp.exp(-0.5 * diff_v * diff_v * inv_var[:, None])).astype(jnp.bfloat16)
    return (profile_u, profile_v, diff_u, diff_v, inv_var)

def block_grads(positions, rotation, amplitudes, widths, residual_b):
    profile_u, profile_v, diff_u, diff_v, inv_var = factors(positions, rotation, amplitudes, widths)
    pu = profile_u.astype(jnp.float32)
    pv = profile_v.astype(jnp.float32)
    rb = residual_b.astype(jnp.float32)
    weighted_u = jnp.dot(pv, rb.T, precision=lax.Precision.HIGHEST, preferred_element_type=jnp.float32)
    weighted_v = jnp.dot(pu, rb, precision=lax.Precision.HIGHEST, preferred_element_type=jnp.float32)
    grad_u = inv_var * lax.optimization_barrier(jnp.sum(pu * diff_u * weighted_u, axis=1))
    grad_v = inv_var * lax.optimization_barrier(jnp.sum(pv * diff_v * weighted_v, axis=1))
    return jnp.stack([rotation[0, c] * grad_u + rotation[1, c] * grad_v for c in range(3)])

def reference(observed, pose_index, batch_order, latents, base_positions, amplitudes, widths, deform_modes):
    blocks = GAUSSIANS // G_DEV
    amp_blocks = amplitudes.reshape(blocks, G_DEV)
    wid_blocks = widths.reshape(blocks, G_DEV)
    current = deform_modes
    finals = []
    for outer in range(STEPS):
        mode_grad = jnp.zeros((K, 3, GAUSSIANS), jnp.float32)
        finals = []
        for member in range(BATCH):
            chosen = member * IMG_DEV + batch_order[member * IMG_DEV + outer]
            rotation = rotation_rows(pose_index[chosen])
            latent = latents[chosen]
            positions = base_positions + jnp.einsum('k,kcg->cg', latent, current, precision=lax.Precision.HIGHEST)
            pos_blocks = positions.reshape(3, blocks, G_DEV).transpose(1, 0, 2)

            def add_block(running, pieces):
                profile_u, profile_v, diff_u, diff_v, inv_var = factors(pieces[0], rotation, pieces[1], pieces[2])
                term = jnp.dot(profile_u.astype(jnp.float32).T, profile_v.astype(jnp.float32), precision=lax.Precision.HIGHEST, preferred_element_type=jnp.float32)
                return (running + term, None)
            image, unused = lax.scan(add_block, jnp.zeros((PIX, PIX), jnp.float32), (pos_blocks, amp_blocks, wid_blocks))
            residual = image - observed[chosen].astype(jnp.float32)
            residual_b = residual.astype(jnp.bfloat16)
            shift_blocks = lax.map(lambda pieces: block_grads(pieces[0], rotation, pieces[1], pieces[2], residual_b), (pos_blocks, amp_blocks, wid_blocks))
            shift_grad = shift_blocks.transpose(1, 0, 2).reshape(3, GAUSSIANS)
            mode_grad = mode_grad + latent[:, None, None] * shift_grad[None]
            finals.append(residual)
        squares = jnp.sum(mode_grad * mode_grad)
        current = current - step_size * mode_grad / jnp.sqrt(squares / (3 * K * GAUSSIANS) + tiny_eps)
    return (jnp.stack(finals), current)
```

```python
import functools
import math

import jax
import jax.numpy as jnp
from jax import lax
from jax.experimental import pallas as pl
from jax.experimental.pallas import tpu as pltpu
from jax.sharding import PartitionSpec as P

NROT = 4096
STEPS = 2
SUB = 8

step_size = 0.5
tiny_eps = 1e-06
LOG2E = 1.4426950408889634


SMEM = pl.BlockSpec(memory_space=pltpu.SMEM)
VMEM = pl.BlockSpec(memory_space=pltpu.VMEM)


def rotation_rows(pose_id):
    cos_beta = 1.0 - (2 * pose_id + 1).astype(jnp.float32) / NROT
    sin_beta = jnp.sqrt(1.0 - cos_beta * cos_beta)
    alpha = (pose_id * 55 % 144).astype(jnp.float32) * (2.0 * math.pi / 144.0)
    gamma = (pose_id % 8).astype(jnp.float32) * (math.pi / 4.0)
    ca, sa = jnp.cos(alpha), jnp.sin(alpha)
    cg, sg = jnp.cos(gamma), jnp.sin(gamma)
    cb, sb = cos_beta, sin_beta
    return jnp.stack(
        [
            ca * cb * cg - sa * sg,
            -ca * cb * sg - sa * cg,
            ca * sb,
            sa * cb * cg + ca * sg,
            -sa * cb * sg + ca * cg,
            sa * sb,
        ],
        axis=-1,
    )


def xor_pairs(n, s):
    return [(i, i ^ s) for i in range(n)]


def exchange(x, axis, s):
    return lax.ppermute(x, axis, xor_pairs(lax.axis_size(axis), s))


def project_kernel(*refs, n_img, k_modes, center):
    me_ref = refs[0]
    pk = refs[1 : 1 + n_img]
    base_ref, modes_ref = refs[1 + n_img : 3 + n_img]
    outs = refs[3 + n_img :]
    own = modes_ref.shape[2]
    lanes = own // SUB
    start = pl.multiple_of(me_ref[0] * own, 128)
    base = base_ref[:, pl.ds(start, own)]
    for s in range(STEPS):
        for t in range(n_img):
            pos = base
            acc = pk[t][s, 0] * modes_ref[0]
            for k in range(1, k_modes):
                acc = acc + pk[t][s, k] * modes_ref[k]
            pos = base + acc
            for r in range(2):
                o = k_modes + 3 * r
                row = (
                    pk[t][s, o] * pos[0:1]
                    + pk[t][s, o + 1] * pos[1:2]
                    + pk[t][s, o + 2] * pos[2:3]
                    + center
                )
                for j in range(SUB):
                    outs[t][s, r, j : j + 1, :] = row[:, j * lanes : (j + 1) * lanes]


def project(me, pk, base, modes, pix):
    n_img = len(pk)
    own = modes.shape[2]
    shape = jax.ShapeDtypeStruct((STEPS, 2, SUB, own // SUB), jnp.float32)
    return pl.pallas_call(
        functools.partial(
            project_kernel, n_img=n_img, k_modes=modes.shape[0], center=(pix - 1) * 0.5
        ),
        out_shape=[shape] * n_img,
        in_specs=[SMEM] * (1 + n_img) + [VMEM, VMEM],
        out_specs=[VMEM] * n_img,
        name="project",
    )(me, *pk, base, modes)


def total_of(s_ref):
    return jnp.sum(jnp.sum(s_ref[...], axis=0, keepdims=True), axis=1, keepdims=True)


def step_length(s_ref, entries):
    return step_size / jnp.sqrt(total_of(s_ref) / entries + tiny_eps)


def forward_kernel(*refs, n_img, outer, entries, rows, nz):
    idx_ref = refs[0]
    p_refs = refs[1 : 1 + n_img]
    pos = 1 + n_img
    if outer:
        q_ref, s_ref = refs[pos : pos + 2]
        pos += 2
    amp_ref, wid_ref, keep_ref, send_ref, proj_ref, par_ref, acc_ref = refs[pos:]
    pix = acc_ref.shape[0]
    lanes = amp_ref.shape[2]
    me = idx_ref[0]
    core = idx_ref[1]
    if outer:
        alpha = step_length(s_ref, entries)
    for t in range(n_img):
        p = p_refs[t][outer]
        if outer:
            p = p - alpha * q_ref[t]
        proj_ref[t] = p
        w = wid_ref[me ^ t]
        inv = 1.0 / (w * w)
        par_ref[t, 0] = (-0.5 * LOG2E) * inv
        par_ref[t, 1] = amp_ref[me ^ t]
    acc_ref[...] = jnp.zeros_like(acc_ref)
    pixels = lax.broadcasted_iota(jnp.int32, (pix, lanes), 0).astype(jnp.float32)

    def slot(t, carry):
        total = None
        for j in range(SUB):
            c = par_ref[t, 0, j : j + 1, :]
            a = par_ref[t, 1, j : j + 1, :]
            du = pixels - proj_ref[t, 0, j : j + 1, :]
            dv = pixels - proj_ref[t, 1, j : j + 1, :]
            u = jnp.exp2(du * du * c).astype(jnp.bfloat16)
            v = (a * jnp.exp2(dv * dv * c)).astype(jnp.bfloat16)
            term = lax.dot_general(
                u, v, (((1,), (1,)), ((), ())), preferred_element_type=jnp.float32
            )
            total = term if total is None else total + term
        acc_ref[...] += total
        return carry

    lax.fori_loop(0, n_img, slot, 0)
    for z in range(nz):
        keep_ref[z] = acc_ref[pl.ds(pl.multiple_of((2 * z + core) * rows, 8), rows), :]
        send_ref[z] = acc_ref[pl.ds(pl.multiple_of((2 * z + 1 - core) * rows, 8), rows), :]


def forward(idx, p_list, q, s_all, amp, wid, outer, entries, pix, rows, nz):
    n_img = len(p_list)
    lanes = amp.shape[2]
    half = jax.ShapeDtypeStruct((nz, rows, pix), jnp.float32)
    proj = jax.ShapeDtypeStruct((n_img, 2, SUB, lanes), jnp.float32)
    extra = [q, s_all] if outer else []
    return pl.pallas_call(
        functools.partial(
            forward_kernel, n_img=n_img, outer=outer, entries=entries, rows=rows, nz=nz
        ),
        out_shape=[half, half, proj],
        in_specs=[SMEM] + [VMEM] * (n_img + len(extra) + 2),
        out_specs=[VMEM] * 3,
        scratch_shapes=[
            pltpu.VMEM((n_img, 2, SUB, lanes), jnp.float32),
            pltpu.VMEM((pix, pix), jnp.float32),
        ],
        name="forward",
    )(idx, *p_list, *extra, amp, wid)


def backward_kernel(idx_ref, own_ref, other_ref, proj_ref, amp_ref, wid_ref, out_ref, par_ref, res_ref, rest_ref, *, n_img, rows, nz):
    pix = res_ref.shape[0]
    lanes = amp_ref.shape[2]
    me = idx_ref[0]
    core = idx_ref[1]
    for t in range(n_img):
        w = wid_ref[me ^ t]
        inv = 1.0 / (w * w)
        par_ref[t, 0] = (-0.5 * LOG2E) * inv
        par_ref[t, 1] = amp_ref[me ^ t]
        par_ref[t, 2] = inv
    for z in range(nz):
        res_ref[pl.ds(pl.multiple_of((2 * z + core) * rows, 16), rows), :] = own_ref[z]
        res_ref[pl.ds(pl.multiple_of((2 * z + 1 - core) * rows, 16), rows), :] = other_ref[z]
    rest_ref[...] = res_ref[...].astype(jnp.float32).T.astype(jnp.bfloat16)
    pixels = lax.broadcasted_iota(jnp.int32, (pix, lanes), 0).astype(jnp.float32)

    def slot(t, carry):
        for j in range(SUB):
            c = par_ref[t, 0, j : j + 1, :]
            a = par_ref[t, 1, j : j + 1, :]
            inv = par_ref[t, 2, j : j + 1, :]
            du = pixels - proj_ref[t, 0, j : j + 1, :]
            dv = pixels - proj_ref[t, 1, j : j + 1, :]
            u = jnp.exp2(du * du * c)
            v = a * jnp.exp2(dv * dv * c)
            wu = jnp.dot(res_ref[...], v.astype(jnp.bfloat16), preferred_element_type=jnp.float32)
            wv = jnp.dot(rest_ref[...], u.astype(jnp.bfloat16), preferred_element_type=jnp.float32)
            out_ref[t, 0, j : j + 1, :] = inv * jnp.sum(u * du * wu, axis=0, keepdims=True)
            out_ref[t, 1, j : j + 1, :] = inv * jnp.sum(v * dv * wv, axis=0, keepdims=True)
        return carry

    lax.fori_loop(0, n_img, slot, 0)


def backward(idx, own, other, proj, amp, wid, pix, rows, nz):
    n_img = proj.shape[0]
    lanes = amp.shape[2]
    return pl.pallas_call(
        functools.partial(backward_kernel, n_img=n_img, rows=rows, nz=nz),
        out_shape=jax.ShapeDtypeStruct((n_img, 2, SUB, lanes), jnp.float32),
        in_specs=[SMEM] + [VMEM] * 5,
        out_specs=VMEM,
        scratch_shapes=[
            pltpu.VMEM((n_img, 3, SUB, lanes), jnp.float32),
            pltpu.VMEM((pix, pix), jnp.bfloat16),
            pltpu.VMEM((pix, pix), jnp.bfloat16),
        ],
        name="backward",
    )(idx, own, other, proj, amp, wid)


def squares_kernel(*refs, n_img, k_modes, outer, with_q):
    pk = refs[:n_img]
    g = refs[n_img : 2 * n_img]
    s_ref = refs[2 * n_img]
    squares = None
    coef = []
    if with_q:
        q_ref = refs[2 * n_img + 1]
        nxt = outer + 1
        for t in range(n_img):
            zz = pk[0][nxt, 0] * pk[t][outer, 0]
            for k in range(1, k_modes):
                zz = zz + pk[0][nxt, k] * pk[t][outer, k]
            rr = []
            for r in range(2):
                for r2 in range(2):
                    d = 0.0
                    for c in range(3):
                        d = d + pk[0][nxt, k_modes + 3 * r + c] * pk[t][outer, k_modes + 3 * r2 + c]
                    rr.append(zz * d)
            coef.append(rr)
    for t0 in range(n_img):
        gu = [g[t][t0 ^ t, 0] for t in range(n_img)]
        gv = [g[t][t0 ^ t, 1] for t in range(n_img)]
        if with_q:
            for r in range(2):
                q = None
                for t in range(n_img):
                    term = coef[t][2 * r] * gu[t] + coef[t][2 * r + 1] * gv[t]
                    q = term if q is None else q + term
                q_ref[t0, r] = q
        for c in range(3):
            shift = [
                pk[t][outer, k_modes + c] * gu[t] + pk[t][outer, k_modes + 3 + c] * gv[t]
                for t in range(n_img)
            ]
            for k in range(k_modes):
                m = pk[0][outer, k] * shift[0]
                for t in range(1, n_img):
                    m = m + pk[t][outer, k] * shift[t]
                squares = m * m if squares is None else squares + m * m
    row = jnp.sum(squares, axis=0, keepdims=True)
    part = row[:, :128]
    for i in range(1, row.shape[1] // 128):
        part = part + row[:, 128 * i : 128 * (i + 1)]
    s_ref[...] = jnp.broadcast_to(part, s_ref.shape)


def squares_of(pk, g, outer, n_gauss, k_modes, with_q):
    n_img = len(pk)
    shapes = [jax.ShapeDtypeStruct((n_gauss, 128), jnp.float32)]
    if with_q:
        shapes.append(jax.ShapeDtypeStruct(g[0].shape, jnp.float32))
    out = pl.pallas_call(
        functools.partial(
            squares_kernel, n_img=n_img, k_modes=k_modes, outer=outer, with_q=with_q
        ),
        out_shape=shapes,
        in_specs=[SMEM] * n_img + [VMEM] * n_img,
        out_specs=[VMEM] * len(shapes),
        name="squares",
    )(*pk, *g)
    s_all = lax.all_to_all(out[0], "gauss", 0, 0, tiled=True)
    return s_all, (out[1] if with_q else None)


def update_kernel(*refs, n_img, k_modes, entries):
    pk = refs[:n_img]
    pos = n_img
    g = [refs[pos + s * n_img : pos + (s + 1) * n_img] for s in range(STEPS)]
    pos += STEPS * n_img
    s_refs = refs[pos : pos + STEPS]
    modes_ref, out_ref, shift_ref = refs[pos + STEPS :]
    lanes = g[0][0].shape[3]
    shifts = []
    for s in range(STEPS):
        alpha = step_length(s_refs[s], entries)
        for t in range(n_img):
            gu = alpha * g[s][t][0, 0]
            gv = alpha * g[s][t][0, 1]
            for c in range(3):
                sh = pk[t][s, k_modes + c] * gu + pk[t][s, k_modes + 3 + c] * gv
                for j in range(SUB):
                    shift_ref[s * n_img + t, c : c + 1, j * lanes : (j + 1) * lanes] = sh[j : j + 1, :]
    for k in range(k_modes):
        m = modes_ref[k]
        for s in range(STEPS):
            d = pk[0][s, k] * shift_ref[s * n_img]
            for t in range(1, n_img):
                d = d + pk[t][s, k] * shift_ref[s * n_img + t]
            m = m - d
        out_ref[k] = m


def update(pk, g, s_all, modes, entries):
    n_img = len(pk)
    own = modes.shape[2]
    lanes = own // SUB
    quarter = lambda t: pl.BlockSpec((1, 2, SUB, lanes), lambda i: (t, 0, 0, 0))
    whole = lambda shape: pl.BlockSpec(shape, lambda i: (0,) * len(shape))
    return pl.pallas_call(
        functools.partial(
            update_kernel, n_img=n_img, k_modes=modes.shape[0], entries=entries
        ),
        grid=(1,),
        out_shape=jax.ShapeDtypeStruct(modes.shape, jnp.float32),
        in_specs=[SMEM] * n_img
        + [quarter(t) for t in range(n_img)] * STEPS
        + [whole(s_all[0].shape)] * STEPS
        + [whole(modes.shape)],
        out_specs=whole(modes.shape),
        scratch_shapes=[pltpu.VMEM((STEPS * n_img, 3, own), jnp.float32)],
        name="update",
    )(*pk, *[x for gs in g for x in gs], *s_all, modes)


def body(
    observed, pose_index, batch_order, latents, base_positions, amplitudes, widths, deform_modes
):
    n_img = lax.axis_size("img")
    n_gauss = lax.axis_size("gauss")
    me = lax.axis_index("img")
    place = lax.axis_index("gauss")
    core = place % 2
    zplace = place // 2
    nz = n_gauss // 2
    per_dev, rows, pix = observed.shape
    k_modes, _, own = deform_modes.shape
    shard = base_positions.shape[1]
    entries = 3 * k_modes * shard * n_gauss
    lanes = own // SUB

    pick = batch_order[:STEPS, None] == jnp.arange(per_dev)[None, :]
    latent = jnp.sum(jnp.where(pick[:, :, None], latents[None], 0.0), axis=1)
    pose = jnp.sum(jnp.where(pick, pose_index[None, :], 0), axis=1)
    pack = jnp.concatenate([latent, rotation_rows(pose)], axis=1)
    pk = [pack] + [exchange(pack, "img", t) for t in range(1, n_img)]

    idx = jnp.stack([me, core]).astype(jnp.int32)
    amp = amplitudes.reshape(n_img, SUB, lanes)
    wid = widths.reshape(n_img, SUB, lanes)

    proj = project(idx, pk, base_positions, deform_modes, pix)
    proj = [proj[0]] + [exchange(proj[t], "img", t) for t in range(1, n_img)]

    mine = (lax.broadcasted_iota(jnp.int32, (nz, 1, 1), 0) == zplace)
    q = None
    grads, sums = [], []
    s_all = None
    for outer in range(STEPS):
        measured = observed[batch_order[outer]].astype(jnp.float32)
        keep, send, here = forward(
            idx, proj, q, s_all, amp, wid, outer, entries, pix, rows, nz
        )
        part = keep + exchange(send, "gauss", 1) - jnp.where(mine, measured[None], 0.0)
        bit = 2
        while bit < n_gauss:
            part = part + exchange(part.astype(jnp.bfloat16), "gauss", bit).astype(jnp.float32)
            bit *= 2
        half = part.astype(jnp.bfloat16)
        other = exchange(half, "gauss", 1)
        g = backward(idx, half, other, here, amp, wid, pix, rows, nz)
        g = [g] + [exchange(g, "img", t) for t in range(1, n_img)]
        s_all, q = squares_of(pk, g, outer, n_gauss, k_modes, outer + 1 < STEPS)
        grads.append(g)
        sums.append(s_all)
    final_rows = lax.dynamic_index_in_dim(part, zplace, 0, keepdims=False)
    out_modes = update(pk, grads, sums, deform_modes, entries)
    return (final_rows[None], out_modes)


def solution(mesh):
    return jax.shard_map(
        body,
        mesh=mesh,
        in_specs=(
            P("img", "gauss", None),
            P("img"),
            P("img"),
            P("img", None),
            P(None, "gauss"),
            P("gauss"),
            P("gauss"),
            P(None, None, ("gauss", "img")),
        ),
        out_specs=(P("img", "gauss", None), P(None, None, ("gauss", "img"))),
        check_vma=False,
    )
```

```python
import functools
import math

import jax
import jax.numpy as jnp
from jax import lax
from jax.experimental import pallas as pl
from jax.experimental.pallas import tpu as pltpu
from jax.sharding import PartitionSpec as P

NROT = 4096
STEPS = 2
SUB = 8

step_size = 0.5
tiny_eps = 1e-06
LOG2E = 1.4426950408889634


SMEM = pl.BlockSpec(memory_space=pltpu.SMEM)
VMEM = pl.BlockSpec(memory_space=pltpu.VMEM)
PARAMS = pltpu.CompilerParams(vmem_limit_bytes=16 << 20)


def xor_pairs(n, s):
    return [(i, i ^ s) for i in range(n)]


def exchange(x, axis, s):
    return lax.ppermute(x, axis, xor_pairs(lax.axis_size(axis), s))


def call(kernel, name, out_shape, args, in_specs=None, scratch=()):
    return pl.pallas_call(
        kernel,
        out_shape=out_shape,
        in_specs=in_specs or [VMEM] * len(args),
        out_specs=jax.tree.map(lambda _: VMEM, out_shape),
        scratch_shapes=list(scratch),
        compiler_params=PARAMS,
        name=name,
    )(*args)


def f32(*shape):
    return jax.ShapeDtypeStruct(shape, jnp.float32)


def pack_kernel(order_ref, pose_ref, latents_ref, out_ref):
    k_modes = latents_ref.shape[1]
    lane = lax.broadcasted_iota(jnp.int32, (1, 128), 1)
    diag = lax.broadcasted_iota(jnp.int32, (k_modes, k_modes), 0) == lax.broadcasted_iota(
        jnp.int32, (k_modes, k_modes), 1
    )
    latent = jnp.zeros((k_modes, 128), jnp.float32)
    pose = jnp.zeros((1, 128), jnp.int32)
    turn = jnp.zeros((1, 128), jnp.int32)
    for s in range(STEPS):
        o = order_ref[s]
        n = pose_ref[o]
        row = latents_ref[pl.ds(o, 1), :]
        col = jnp.sum(
            jnp.where(diag, jnp.broadcast_to(row, diag.shape), 0.0), axis=1, keepdims=True
        )
        latent = jnp.where(lane == s, col, latent)
        pose = jnp.where(lane == s, n, pose)
        turn = jnp.where(lane == s, lax.rem(n * 55, 144), turn)
    cb = 1.0 - (2 * pose + 1).astype(jnp.float32) / NROT
    sb = jnp.sqrt(1.0 - cb * cb)
    alpha = turn.astype(jnp.float32) * (2.0 * math.pi / 144.0)
    gamma = (pose & 7).astype(jnp.float32) * (math.pi / 4.0)
    ca, sa = jnp.cos(alpha), jnp.sin(alpha)
    cg, sg = jnp.cos(gamma), jnp.sin(gamma)
    rows = [
        ca * cb * cg - sa * sg,
        -ca * cb * sg - sa * cg,
        ca * sb,
        sa * cb * cg + ca * sg,
        -sa * cb * sg + ca * cg,
        sa * sb,
    ]
    out_ref[0:k_modes, :] = latent
    for i, row in enumerate(rows):
        out_ref[k_modes + i : k_modes + i + 1, :] = row
    out_ref[k_modes + 6 :, :] = jnp.zeros((2, 128), jnp.float32)


def prepare_kernel(order_ref, observed_ref, amp_ref, wid_ref, par_ref, obs_ref):
    n_img, _, sub, lanes = par_ref.shape
    me = lax.axis_index("img")
    for s in range(STEPS):
        obs_ref[s] = observed_ref[order_ref[s]].astype(jnp.float32)
    for t in range(n_img):
        for j in range(sub):
            at = pl.multiple_of(((me ^ t) * sub + j) * lanes, lanes)
            w = wid_ref[pl.ds(at, lanes)].reshape(1, lanes)
            inv = 1.0 / (w * w)
            par_ref[t, 0, j : j + 1, :] = (-0.5 * LOG2E) * inv
            par_ref[t, 1, j : j + 1, :] = amp_ref[pl.ds(at, lanes)].reshape(1, lanes)
            par_ref[t, 2, j : j + 1, :] = inv


def project_kernel(*refs, n_img, center):
    pk = refs[:n_img]
    base_ref, modes_ref = refs[n_img : n_img + 2]
    outs = refs[n_img + 2 :]
    _, k_modes, own = modes_ref.shape
    lanes = own // SUB
    start = pl.multiple_of(lax.axis_index("img") * own, own)
    base = [base_ref[c : c + 1, pl.ds(start, own)] for c in range(3)]
    for s in range(STEPS):
        for t in range(n_img):
            col = jnp.broadcast_to(pk[t][0:k_modes, s : s + 1], (k_modes, own))
            pos = [
                base[c] + jnp.sum(col * modes_ref[c], axis=0, keepdims=True) for c in range(3)
            ]
            for r in range(2):
                o = k_modes + 3 * r
                row = (
                    pk[t][o : o + 1, s : s + 1] * pos[0]
                    + pk[t][o + 1 : o + 2, s : s + 1] * pos[1]
                    + pk[t][o + 2 : o + 3, s : s + 1] * pos[2]
                    + center
                )
                for j in range(SUB):
                    outs[t][s, r, j : j + 1, :] = row[:, j * lanes : (j + 1) * lanes]


def spread_kernel(*refs, n_img, k_modes):
    pk = refs[:n_img]
    z_ref, r_ref, c_ref = refs[n_img:]
    lanes = z_ref.shape[3]
    for s in range(STEPS):
        for t in range(n_img):
            z_ref[s, t] = jnp.broadcast_to(pk[t][0:k_modes, s : s + 1], (k_modes, lanes))
            r_ref[s, t] = jnp.broadcast_to(pk[t][k_modes : k_modes + 8, s : s + 1], (8, lanes))
    for s in range(STEPS - 1):
        for t in range(n_img):
            zz = jnp.sum(z_ref[s + 1, 0] * z_ref[s, t], axis=0, keepdims=True)
            for r in range(2):
                for r2 in range(2):
                    d = None
                    for c in range(3):
                        e = (
                            r_ref[s + 1, 0, 3 * r + c : 3 * r + c + 1]
                            * r_ref[s, t, 3 * r2 + c : 3 * r2 + c + 1]
                        )
                        d = e if d is None else d + e
                    i = 2 * r + r2
                    c_ref[s, t, i : i + 1] = zz * d


def total_of(s_ref):
    return jnp.sum(jnp.sum(s_ref[...], axis=0, keepdims=True), axis=1, keepdims=True)


def step_length(s_ref, entries):
    return step_size / jnp.sqrt(total_of(s_ref) / entries + tiny_eps)


def forward_kernel(*refs, n_img, outer, entries, rows, nz):
    p_refs = refs[:n_img]
    pos = n_img
    if outer:
        q_ref, s_ref = refs[pos : pos + 2]
        pos += 2
    par_ref, obs_ref, keep_ref, send_ref, proj_ref, acc_ref, pix_ref = refs[pos:]
    pix, lanes = pix_ref.shape
    place = lax.axis_index("gauss")
    core = place % 2
    if outer:
        alpha = step_length(s_ref, entries)
    for t in range(n_img):
        p = p_refs[t][outer]
        if outer:
            p = p - alpha * q_ref[t]
        proj_ref[t] = p
    pix_ref[...] = lax.broadcasted_iota(jnp.int32, (pix, lanes), 0).astype(jnp.float32)
    acc_ref[...] = jnp.zeros_like(acc_ref)

    def slot(t, carry):
        total = None
        for j in range(SUB):
            c = par_ref[t, 0, j : j + 1, :]
            a = par_ref[t, 1, j : j + 1, :]
            du = pix_ref[...] - proj_ref[t, 0, j : j + 1, :]
            dv = pix_ref[...] - proj_ref[t, 1, j : j + 1, :]
            u = jnp.exp2(du * du * c).astype(jnp.bfloat16)
            v = (a * jnp.exp2(dv * dv * c)).astype(jnp.bfloat16)
            term = lax.dot_general(
                u, v, (((1,), (1,)), ((), ())), preferred_element_type=jnp.float32
            )
            total = term if total is None else total + term
        acc_ref[...] += total
        return carry

    lax.fori_loop(0, n_img, slot, 0)
    for z in range(nz):
        keep_ref[z] = acc_ref[pl.ds(pl.multiple_of((2 * z + core) * rows, 8), rows), :]
        send_ref[z] = acc_ref[pl.ds(pl.multiple_of((2 * z + 1 - core) * rows, 8), rows), :]
    keep_ref[place // 2] -= obs_ref[outer]


def backward_kernel(
    own_ref, other_ref, proj_ref, par_ref, out_ref, res_ref, rest_ref, pix_ref, *, n_img, rows, nz
):
    pix, lanes = pix_ref.shape
    core = lax.axis_index("gauss") % 2
    for z in range(nz):
        res_ref[pl.ds(pl.multiple_of((2 * z + core) * rows, 16), rows), :] = own_ref[z]
        res_ref[pl.ds(pl.multiple_of((2 * z + 1 - core) * rows, 16), rows), :] = other_ref[z]
    rest_ref[...] = res_ref[...].astype(jnp.float32).T.astype(jnp.bfloat16)
    pix_ref[...] = lax.broadcasted_iota(jnp.int32, (pix, lanes), 0).astype(jnp.float32)

    def slot(t, carry):
        for j in range(SUB):
            c = par_ref[t, 0, j : j + 1, :]
            a = par_ref[t, 1, j : j + 1, :]
            inv = par_ref[t, 2, j : j + 1, :]
            du = pix_ref[...] - proj_ref[t, 0, j : j + 1, :]
            dv = pix_ref[...] - proj_ref[t, 1, j : j + 1, :]
            u = jnp.exp2(du * du * c)
            v = a * jnp.exp2(dv * dv * c)
            wu = jnp.dot(res_ref[...], v.astype(jnp.bfloat16), preferred_element_type=jnp.float32)
            wv = jnp.dot(rest_ref[...], u.astype(jnp.bfloat16), preferred_element_type=jnp.float32)
            out_ref[t, 0, j : j + 1, :] = inv * jnp.sum(u * du * wu, axis=0, keepdims=True)
            out_ref[t, 1, j : j + 1, :] = inv * jnp.sum(v * dv * wv, axis=0, keepdims=True)
        return carry

    lax.fori_loop(0, n_img, slot, 0)


def shifts_of(r_ref, s, t, gu, gv, c):
    return r_ref[s, t, c : c + 1] * gu + r_ref[s, t, 3 + c : 4 + c] * gv


def squares_kernel(*refs, n_img, outer, with_q):
    z_ref, r_ref, c_ref = refs[:3]
    g = refs[3 : 3 + n_img]
    outs = refs[3 + n_img :]
    s_ref, shift_ref = outs[0], outs[-1]
    k_modes, lanes = z_ref.shape[2:]
    z = [z_ref[outer, t] for t in range(n_img)]
    squares = jnp.zeros((k_modes, lanes), jnp.float32)
    for t0 in range(n_img):
        gu = [g[t][t0 ^ t, 0] for t in range(n_img)]
        gv = [g[t][t0 ^ t, 1] for t in range(n_img)]
        for r in range(2 if with_q else 0):
            q = None
            for t in range(n_img):
                e = (
                    c_ref[outer, t, 2 * r : 2 * r + 1] * gu[t]
                    + c_ref[outer, t, 2 * r + 1 : 2 * r + 2] * gv[t]
                )
                q = e if q is None else q + e
            outs[1][t0, r] = q
        for c in range(3):
            for t in range(n_img):
                shift_ref[t0, c, t] = shifts_of(r_ref, outer, t, gu[t], gv[t], c)
    for t0 in range(n_img):
        for c in range(3):
            for j in range(SUB):
                m = None
                for t in range(n_img):
                    e = z[t] * shift_ref[t0, c, t, j : j + 1]
                    m = e if m is None else m + e
                squares = squares + m * m
    row = jnp.sum(squares, axis=0, keepdims=True)
    part = row[:, :128]
    for i in range(1, lanes // 128):
        part = part + row[:, 128 * i : 128 * (i + 1)]
    s_ref[...] = jnp.broadcast_to(part, s_ref.shape)


def update_kernel(*refs, n_img, entries):
    z_ref, r_ref = refs[:2]
    pos = 2
    g = [refs[pos + s * n_img : pos + (s + 1) * n_img] for s in range(STEPS)]
    pos += STEPS * n_img
    s_refs = refs[pos : pos + STEPS]
    modes_ref, out_ref, shift_ref = refs[pos + STEPS :]
    lanes = z_ref.shape[3]
    for s in range(STEPS):
        alpha = step_length(s_refs[s], entries)
        for t in range(n_img):
            gu = alpha * g[s][t][t, 0]
            gv = alpha * g[s][t][t, 1]
            for c in range(3):
                shift_ref[s, t, c] = shifts_of(r_ref, s, t, gu, gv, c)
    for c in range(3):
        for j in range(SUB):
            m = modes_ref[c, :, j * lanes : (j + 1) * lanes]
            for s in range(STEPS):
                for t in range(n_img):
                    m = m - z_ref[s, t] * shift_ref[s, t, c, j : j + 1]
            out_ref[c, :, j * lanes : (j + 1) * lanes] = m


def body(
    observed, pose_index, batch_order, latents, base_positions, amplitudes, widths, deform_modes
):
    n_img = lax.axis_size("img")
    n_gauss = lax.axis_size("gauss")
    zplace = lax.axis_index("gauss") // 2
    nz = n_gauss // 2
    _, rows, pix = observed.shape
    k_modes, _, own = deform_modes.shape
    entries = 3 * k_modes * base_positions.shape[1] * n_gauss
    lanes = own // SUB
    modes = jnp.transpose(deform_modes, (1, 0, 2))
    part_fn = functools.partial

    pack = call(
        pack_kernel, "pack", f32(k_modes + 8, 128), (batch_order, pose_index, latents),
        [SMEM, SMEM, VMEM],
    )
    pk = [pack] + [exchange(pack, "img", t) for t in range(1, n_img)]
    par, obs = call(
        prepare_kernel, "prepare", [f32(n_img, 3, SUB, lanes), f32(STEPS, rows, pix)],
        (batch_order, observed, amplitudes, widths), [SMEM, VMEM, VMEM, VMEM],
    )
    proj = call(
        part_fn(project_kernel, n_img=n_img, center=(pix - 1) * 0.5), "project",
        [f32(STEPS, 2, SUB, lanes)] * n_img, (*pk, base_positions, modes),
    )
    proj = [proj[0]] + [exchange(proj[t], "img", t) for t in range(1, n_img)]
    zs, rs, cs = call(
        part_fn(spread_kernel, n_img=n_img, k_modes=k_modes), "spread",
        [f32(STEPS, n_img, k_modes, lanes), f32(STEPS, n_img, 8, lanes),
         f32(STEPS - 1, n_img, 8, lanes)],
        pk,
    )

    extra = []
    grads, sums = [], []
    half_shape = f32(nz, rows, pix)
    per_shard = f32(n_img, 2, SUB, lanes)
    for outer in range(STEPS):
        keep, send, here = call(
            part_fn(forward_kernel, n_img=n_img, outer=outer, entries=entries, rows=rows, nz=nz),
            "forward", [half_shape, half_shape, per_shard], (*proj, *extra, par, obs),
            scratch=[pltpu.VMEM((pix, pix), jnp.float32), pltpu.VMEM((pix, lanes), jnp.float32)],
        )
        part = keep + exchange(send, "gauss", 1)
        bit = 2
        while bit < n_gauss:
            part = part + exchange(part.astype(jnp.bfloat16), "gauss", bit).astype(jnp.float32)
            bit *= 2
        half = part.astype(jnp.bfloat16)
        other = exchange(half, "gauss", 1)
        g = call(
            part_fn(backward_kernel, n_img=n_img, rows=rows, nz=nz), "backward", per_shard,
            (half, other, here, par),
            scratch=[pltpu.VMEM((pix, pix), jnp.bfloat16)] * 2
            + [pltpu.VMEM((pix, lanes), jnp.float32)],
        )
        g = [g] + [exchange(g, "img", t) for t in range(1, n_img)]
        more = outer + 1 < STEPS
        out = call(
            part_fn(squares_kernel, n_img=n_img, outer=outer, with_q=more), "squares",
            [f32(n_gauss, 128)] + [per_shard] * more, (zs, rs, cs, *g),
            scratch=[pltpu.VMEM((n_img, 3, n_img, SUB, lanes), jnp.float32)],
        )
        s_all = lax.all_to_all(out[0], "gauss", 0, 0, tiled=True)
        extra = [out[-1], s_all]
        grads.extend(g)
        sums.append(s_all)
    final_rows = lax.dynamic_index_in_dim(part, zplace, 0, keepdims=False)
    new = call(
        part_fn(update_kernel, n_img=n_img, entries=entries), "update", f32(*modes.shape),
        (zs, rs, *grads, *sums, modes),
        scratch=[pltpu.VMEM((STEPS, n_img, 3, SUB, lanes), jnp.float32)],
    )
    return (final_rows[None], jnp.transpose(new, (1, 0, 2)))


def solution(mesh):
    return jax.shard_map(
        body,
        mesh=mesh,
        in_specs=(
            P("img", "gauss", None),
            P("img"),
            P("img"),
            P("img", None),
            P(None, "gauss"),
            P("gauss"),
            P("gauss"),
            P(None, None, ("gauss", "img")),
        ),
        out_specs=(P("img", "gauss", None), P(None, None, ("gauss", "img"))),
        check_vma=False,
    )
```

```python
import functools
import math

import jax
import jax.numpy as jnp
from jax import lax
from jax.experimental import pallas as pl
from jax.experimental.pallas import tpu as pltpu
from jax.sharding import PartitionSpec as P

NROT = 4096
STEPS = 2
SUB = 8

step_size = 0.5
tiny_eps = 1e-06
LOG2E = 1.4426950408889634


SMEM = pl.BlockSpec(memory_space=pltpu.SMEM)
VMEM = pl.BlockSpec(memory_space=pltpu.VMEM)
HBM = pl.BlockSpec(memory_space=pltpu.HBM)
PARAMS = pltpu.CompilerParams(vmem_limit_bytes=16 << 20)


def xor_pairs(n, s):
    return [(i, i ^ s) for i in range(n)]


def exchange(x, axis, s):
    return lax.ppermute(x, axis, xor_pairs(lax.axis_size(axis), s))


def call(kernel, name, out_shape, args, in_specs=None, scratch=()):
    return pl.pallas_call(
        kernel,
        out_shape=out_shape,
        in_specs=in_specs or [VMEM] * len(args),
        out_specs=jax.tree.map(lambda _: VMEM, out_shape),
        scratch_shapes=list(scratch),
        compiler_params=PARAMS,
        name=name,
    )(*args)


def f32(*shape):
    return jax.ShapeDtypeStruct(shape, jnp.float32)


def load(pairs, sem):
    copies = [pltpu.make_async_copy(a, b, sem.at[i]) for i, (a, b) in enumerate(pairs)]
    for copy in copies:
        copy.start()
    for copy in copies:
        copy.wait()


def pack_kernel(order_in, pose_in, latents_in, out_ref, order_ref, pose_ref, latents_ref, sem):
    load([(order_in, order_ref), (pose_in, pose_ref), (latents_in, latents_ref)], sem)
    k_modes = latents_ref.shape[1]
    lane = lax.broadcasted_iota(jnp.int32, (1, 128), 1)
    diag = lax.broadcasted_iota(jnp.int32, (k_modes, k_modes), 0) == lax.broadcasted_iota(
        jnp.int32, (k_modes, k_modes), 1
    )
    latent = jnp.zeros((k_modes, 128), jnp.float32)
    pose = jnp.zeros((1, 128), jnp.int32)
    turn = jnp.zeros((1, 128), jnp.int32)
    for s in range(STEPS):
        o = order_ref[s]
        n = pose_ref[o]
        row = latents_ref[pl.ds(o, 1), :]
        col = jnp.sum(
            jnp.where(diag, jnp.broadcast_to(row, diag.shape), 0.0), axis=1, keepdims=True
        )
        latent = jnp.where(lane == s, col, latent)
        pose = jnp.where(lane == s, n, pose)
        turn = jnp.where(lane == s, lax.rem(n * 55, 144), turn)
    cb = 1.0 - (2 * pose + 1).astype(jnp.float32) / NROT
    sb = jnp.sqrt(1.0 - cb * cb)
    alpha = turn.astype(jnp.float32) * (2.0 * math.pi / 144.0)
    gamma = (pose & 7).astype(jnp.float32) * (math.pi / 4.0)
    ca, sa = jnp.cos(alpha), jnp.sin(alpha)
    cg, sg = jnp.cos(gamma), jnp.sin(gamma)
    rows = [
        ca * cb * cg - sa * sg,
        -ca * cb * sg - sa * cg,
        ca * sb,
        sa * cb * cg + ca * sg,
        -sa * cb * sg + ca * cg,
        sa * sb,
    ]
    out_ref[0:k_modes, :] = latent
    for i, row in enumerate(rows):
        out_ref[k_modes + i : k_modes + i + 1, :] = row
    out_ref[k_modes + 6 :, :] = jnp.zeros((2, 128), jnp.float32)


def prepare_kernel(
    order_in, observed_in, amp_in, wid_in, base_in, modes_in,
    par_ref, obs_ref, base_ref, modes_ref,
    order_ref, observed_ref, amp_ref, wid_ref, sem,
):
    n_img, _, sub, lanes = par_ref.shape
    own = sub * lanes
    me = lax.axis_index("img")
    start = pl.multiple_of(me * own, own)
    load(
        [
            (order_in, order_ref),
            (observed_in, observed_ref),
            (amp_in, amp_ref),
            (wid_in, wid_ref),
            (base_in.at[:, pl.ds(start, own)], base_ref),
            (modes_in, modes_ref),
        ],
        sem,
    )
    for s in range(STEPS):
        obs_ref[s] = observed_ref[order_ref[s]].astype(jnp.float32)
    for t in range(n_img):
        for j in range(sub):
            at = pl.multiple_of(((me ^ t) * sub + j) * lanes, lanes)
            w = wid_ref[pl.ds(at, lanes)].reshape(1, lanes)
            inv = 1.0 / (w * w)
            par_ref[t, 0, j : j + 1, :] = (-0.5 * LOG2E) * inv
            par_ref[t, 1, j : j + 1, :] = amp_ref[pl.ds(at, lanes)].reshape(1, lanes)
            par_ref[t, 2, j : j + 1, :] = inv


def project_kernel(*refs, n_img, center):
    pk = refs[:n_img]
    base_ref, modes_ref = refs[n_img : n_img + 2]
    outs = refs[n_img + 2 :]
    _, k_modes, own = modes_ref.shape
    lanes = own // SUB
    base = [base_ref[c : c + 1, :] for c in range(3)]
    for s in range(STEPS):
        for t in range(n_img):
            col = jnp.broadcast_to(pk[t][0:k_modes, s : s + 1], (k_modes, own))
            pos = [
                base[c] + jnp.sum(col * modes_ref[c], axis=0, keepdims=True) for c in range(3)
            ]
            for r in range(2):
                o = k_modes + 3 * r
                row = (
                    pk[t][o : o + 1, s : s + 1] * pos[0]
                    + pk[t][o + 1 : o + 2, s : s + 1] * pos[1]
                    + pk[t][o + 2 : o + 3, s : s + 1] * pos[2]
                    + center
                )
                for j in range(SUB):
                    outs[t][s, r, j : j + 1, :] = row[:, j * lanes : (j + 1) * lanes]


def spread_kernel(*refs, n_img, k_modes):
    pk = refs[:n_img]
    z_ref, r_ref, c_ref = refs[n_img:]
    lanes = z_ref.shape[3]
    for s in range(STEPS):
        for t in range(n_img):
            z_ref[s, t] = jnp.broadcast_to(pk[t][0:k_modes, s : s + 1], (k_modes, lanes))
            r_ref[s, t] = jnp.broadcast_to(pk[t][k_modes : k_modes + 8, s : s + 1], (8, lanes))
    for s in range(STEPS - 1):
        for t in range(n_img):
            zz = jnp.sum(z_ref[s + 1, 0] * z_ref[s, t], axis=0, keepdims=True)
            for r in range(2):
                for r2 in range(2):
                    d = None
                    for c in range(3):
                        e = (
                            r_ref[s + 1, 0, 3 * r + c : 3 * r + c + 1]
                            * r_ref[s, t, 3 * r2 + c : 3 * r2 + c + 1]
                        )
                        d = e if d is None else d + e
                    i = 2 * r + r2
                    c_ref[s, t, i : i + 1] = zz * d


def step_length(s_refs, entries):
    total = s_refs[0][...]
    for ref in s_refs[1:]:
        total = total + ref[...]
    total = jnp.sum(jnp.sum(total, axis=0, keepdims=True), axis=1, keepdims=True)
    return step_size / jnp.sqrt(total / entries + tiny_eps)


def forward_kernel(*refs, n_img, outer, entries, rows, nz):
    p_refs = refs[:n_img]
    pos = n_img
    if outer:
        q_ref = refs[pos]
        s_refs = refs[pos + 1 : pos + 1 + nz]
        pos += 1 + nz
    par_ref, obs_ref, keep_ref, send_ref, proj_ref, u_ref, v_ref, acc_ref, pix_ref = refs[pos:]
    pix, lanes = pix_ref.shape
    place = lax.axis_index("gauss")
    core = place % 2
    if outer:
        alpha = step_length(s_refs, entries)
    for t in range(n_img):
        p = p_refs[t][outer]
        if outer:
            p = p - alpha * q_ref[t]
        proj_ref[t] = p
    pix_ref[...] = lax.broadcasted_iota(jnp.int32, (pix, lanes), 0).astype(jnp.float32)
    acc_ref[...] = jnp.zeros_like(acc_ref)

    def slot(t, carry):
        total = None
        for j in range(SUB):
            c = par_ref[t, 0, j : j + 1, :]
            a = par_ref[t, 1, j : j + 1, :]
            du = pix_ref[...] - proj_ref[t, 0, j : j + 1, :]
            dv = pix_ref[...] - proj_ref[t, 1, j : j + 1, :]
            u = jnp.exp2(du * du * c).astype(jnp.bfloat16)
            v = (a * jnp.exp2(dv * dv * c)).astype(jnp.bfloat16)
            u_ref[t, j] = u
            v_ref[t, j] = v
            term = lax.dot_general(
                u, v, (((1,), (1,)), ((), ())), preferred_element_type=jnp.float32
            )
            total = term if total is None else total + term
        acc_ref[...] += total
        return carry

    lax.fori_loop(0, n_img, slot, 0)
    for z in range(nz):
        keep_ref[z] = acc_ref[pl.ds(pl.multiple_of((2 * z + core) * rows, 8), rows), :]
        send_ref[z] = acc_ref[pl.ds(pl.multiple_of((2 * z + 1 - core) * rows, 8), rows), :]
    keep_ref[place // 2] -= obs_ref[outer]


def backward_kernel(
    own_ref, other_ref, proj_ref, par_ref, u_ref, v_ref, out_ref, res_ref, rest_ref, pix_ref,
    *, n_img, rows, nz
):
    pix, lanes = pix_ref.shape
    core = lax.axis_index("gauss") % 2
    for z in range(nz):
        res_ref[pl.ds(pl.multiple_of((2 * z + core) * rows, 16), rows), :] = own_ref[z]
        res_ref[pl.ds(pl.multiple_of((2 * z + 1 - core) * rows, 16), rows), :] = other_ref[z]
    rest_ref[...] = res_ref[...].astype(jnp.float32).T.astype(jnp.bfloat16)
    pix_ref[...] = lax.broadcasted_iota(jnp.int32, (pix, lanes), 0).astype(jnp.float32)

    def slot(t, carry):
        for j in range(SUB):
            inv = par_ref[t, 2, j : j + 1, :]
            u = u_ref[t, j]
            v = v_ref[t, j]
            du = pix_ref[...] - proj_ref[t, 0, j : j + 1, :]
            dv = pix_ref[...] - proj_ref[t, 1, j : j + 1, :]
            wu = jnp.dot(res_ref[...], v, preferred_element_type=jnp.float32)
            wv = jnp.dot(rest_ref[...], u, preferred_element_type=jnp.float32)
            u = u.astype(jnp.float32)
            v = v.astype(jnp.float32)
            out_ref[t, 0, j : j + 1, :] = inv * jnp.sum(u * du * wu, axis=0, keepdims=True)
            out_ref[t, 1, j : j + 1, :] = inv * jnp.sum(v * dv * wv, axis=0, keepdims=True)
        return carry

    lax.fori_loop(0, n_img, slot, 0)


def shifts_of(r_ref, s, t, gu, gv, c):
    return r_ref[s, t, c : c + 1] * gu + r_ref[s, t, 3 + c : 4 + c] * gv


def squares_kernel(*refs, n_img, outer, with_q):
    z_ref, r_ref, c_ref = refs[:3]
    g = refs[3 : 3 + n_img]
    outs = refs[3 + n_img :]
    s_ref, shift_ref = outs[0], outs[-1]
    k_modes, lanes = z_ref.shape[2:]
    z = [z_ref[outer, t] for t in range(n_img)]
    squares = jnp.zeros((k_modes, lanes), jnp.float32)
    for t0 in range(n_img):
        gu = [g[t][t0 ^ t, 0] for t in range(n_img)]
        gv = [g[t][t0 ^ t, 1] for t in range(n_img)]
        for r in range(2 if with_q else 0):
            q = None
            for t in range(n_img):
                e = (
                    c_ref[outer, t, 2 * r : 2 * r + 1] * gu[t]
                    + c_ref[outer, t, 2 * r + 1 : 2 * r + 2] * gv[t]
                )
                q = e if q is None else q + e
            outs[1][t0, r] = q
        for c in range(3):
            for t in range(n_img):
                shift_ref[t0, c, t] = shifts_of(r_ref, outer, t, gu[t], gv[t], c)
    for t0 in range(n_img):
        for c in range(3):
            for j in range(SUB):
                m = None
                for t in range(n_img):
                    e = z[t] * shift_ref[t0, c, t, j : j + 1]
                    m = e if m is None else m + e
                squares = squares + m * m
    part = None
    for k in range(0, k_modes, SUB):
        for i in range(0, lanes, 128):
            e = squares[k : k + SUB, i : i + 128]
            part = e if part is None else part + e
    s_ref[...] = part


def update_kernel(*refs, n_img, nz, entries):
    z_ref, r_ref = refs[:2]
    pos = 2
    g = [refs[pos + s * n_img : pos + (s + 1) * n_img] for s in range(STEPS)]
    pos += STEPS * n_img
    s_refs = [refs[pos + s * nz : pos + (s + 1) * nz] for s in range(STEPS)]
    modes_ref, out_ref, shift_ref = refs[pos + STEPS * nz :]
    lanes = z_ref.shape[3]
    for s in range(STEPS):
        alpha = step_length(s_refs[s], entries)
        for t in range(n_img):
            gu = alpha * g[s][t][t, 0]
            gv = alpha * g[s][t][t, 1]
            for c in range(3):
                shift_ref[s, t, c] = shifts_of(r_ref, s, t, gu, gv, c)
    for c in range(3):
        for j in range(SUB):
            m = modes_ref[c, :, j * lanes : (j + 1) * lanes]
            for s in range(STEPS):
                for t in range(n_img):
                    m = m - z_ref[s, t] * shift_ref[s, t, c, j : j + 1]
            out_ref[c, :, j * lanes : (j + 1) * lanes] = m


def body(
    observed, pose_index, batch_order, latents, base_positions, amplitudes, widths, deform_modes
):
    n_img = lax.axis_size("img")
    n_gauss = lax.axis_size("gauss")
    zplace = lax.axis_index("gauss") // 2
    nz = n_gauss // 2
    _, rows, pix = observed.shape
    k_modes, _, own = deform_modes.shape
    entries = 3 * k_modes * base_positions.shape[1] * n_gauss
    lanes = own // SUB
    modes = jnp.transpose(deform_modes, (1, 0, 2))
    part_fn = functools.partial

    pack = call(
        pack_kernel, "pack", f32(k_modes + 8, 128), (batch_order, pose_index, latents), [HBM] * 3,
        [pltpu.SMEM(batch_order.shape, jnp.int32), pltpu.SMEM(pose_index.shape, jnp.int32),
         pltpu.VMEM(latents.shape, jnp.float32), pltpu.SemaphoreType.DMA((3,))],
    )
    pk = [pack] + [exchange(pack, "img", t) for t in range(1, n_img)]
    par, obs, base, modes = call(
        prepare_kernel, "prepare",
        [f32(n_img, 3, SUB, lanes), f32(STEPS, rows, pix), f32(3, own), f32(3, k_modes, own)],
        (batch_order, observed, amplitudes, widths, base_positions, modes), [HBM] * 6,
        [pltpu.SMEM(batch_order.shape, jnp.int32), pltpu.VMEM(observed.shape, observed.dtype),
         pltpu.VMEM(amplitudes.shape, jnp.float32), pltpu.VMEM(widths.shape, jnp.float32),
         pltpu.SemaphoreType.DMA((6,))],
    )
    proj = call(
        part_fn(project_kernel, n_img=n_img, center=(pix - 1) * 0.5), "project",
        [f32(STEPS, 2, SUB, lanes)] * n_img, (*pk, base, modes),
    )
    proj = [proj[0]] + [exchange(proj[t], "img", t) for t in range(1, n_img)]
    zs, rs, cs = call(
        part_fn(spread_kernel, n_img=n_img, k_modes=k_modes), "spread",
        [f32(STEPS, n_img, k_modes, lanes), f32(STEPS, n_img, 8, lanes),
         f32(STEPS - 1, n_img, 8, lanes)],
        pk,
    )

    extra = []
    grads, sums = [], []
    half_shape = f32(nz, rows, pix)
    per_shard = f32(n_img, 2, SUB, lanes)
    profile = jax.ShapeDtypeStruct((n_img, SUB, pix, lanes), jnp.bfloat16)
    for outer in range(STEPS):
        keep, send, here, u, v = call(
            part_fn(forward_kernel, n_img=n_img, outer=outer, entries=entries, rows=rows, nz=nz),
            "forward", [half_shape, half_shape, per_shard, profile, profile], (*proj, *extra, par, obs),
            scratch=[pltpu.VMEM((pix, pix), jnp.float32), pltpu.VMEM((pix, lanes), jnp.float32)],
        )
        part = keep + exchange(send, "gauss", 1)
        bit = 2
        while bit < n_gauss:
            part = part + exchange(part.astype(jnp.bfloat16), "gauss", bit).astype(jnp.float32)
            bit *= 2
        half = part.astype(jnp.bfloat16)
        other = exchange(half, "gauss", 1)
        g = call(
            part_fn(backward_kernel, n_img=n_img, rows=rows, nz=nz), "backward", per_shard,
            (half, other, here, par, u, v),
            scratch=[pltpu.VMEM((pix, pix), jnp.bfloat16)] * 2
            + [pltpu.VMEM((pix, lanes), jnp.float32)],
        )
        g = [g] + [exchange(g, "img", t) for t in range(1, n_img)]
        more = outer + 1 < STEPS
        out = call(
            part_fn(squares_kernel, n_img=n_img, outer=outer, with_q=more), "squares",
            [f32(SUB, 128)] + [per_shard] * more, (zs, rs, cs, *g),
            scratch=[pltpu.VMEM((n_img, 3, n_img, SUB, lanes), jnp.float32)],
        )
        s_chip = out[0] + exchange(out[0], "gauss", 1)
        s_all = [s_chip] + [exchange(s_chip, "gauss", 2 * t) for t in range(1, nz)]
        extra = [out[-1], *s_all]
        grads.extend(g)
        sums.extend(s_all)
    final_rows = lax.dynamic_index_in_dim(part, zplace, 0, keepdims=False)
    new = call(
        part_fn(update_kernel, n_img=n_img, nz=nz, entries=entries), "update", f32(*modes.shape),
        (zs, rs, *grads, *sums, modes),
        scratch=[pltpu.VMEM((STEPS, n_img, 3, SUB, lanes), jnp.float32)],
    )
    return (final_rows[None], jnp.transpose(new, (1, 0, 2)))


def solution(mesh):
    return jax.shard_map(
        body,
        mesh=mesh,
        in_specs=(
            P("img", "gauss", None),
            P("img"),
            P("img"),
            P("img", None),
            P(None, "gauss"),
            P("gauss"),
            P("gauss"),
            P(None, None, ("gauss", "img")),
        ),
        out_specs=(P("img", "gauss", None), P(None, None, ("gauss", "img"))),
        check_vma=False,
    )
```

```python
import functools
import math

import jax
import jax.numpy as jnp
from jax import lax
from jax.experimental import pallas as pl
from jax.experimental.pallas import tpu as pltpu
from jax.sharding import PartitionSpec as P

NROT = 4096
STEPS = 2
SUB = 8

step_size = 0.5
tiny_eps = 1e-06
LOG2E = 1.4426950408889634


SMEM = pl.BlockSpec(memory_space=pltpu.SMEM)
VMEM = pl.BlockSpec(memory_space=pltpu.VMEM)
HBM = pl.BlockSpec(memory_space=pltpu.HBM)
PARAMS = pltpu.CompilerParams(vmem_limit_bytes=16 << 20)


def xor_pairs(n, s):
    return [(i, i ^ s) for i in range(n)]


def exchange(x, axis, s):
    return lax.ppermute(x, axis, xor_pairs(lax.axis_size(axis), s))


def spread_out(parts, axis, unit=1):
    far_first = range(len(parts) - 1, 0, -1)
    got = {t: exchange(parts[t], axis, t * unit) for t in far_first}
    return [parts[0]] + [got[t] for t in range(1, len(parts))]


def call(kernel, name, out_shape, args, in_specs=None, scratch=()):
    return pl.pallas_call(
        kernel,
        out_shape=out_shape,
        in_specs=in_specs or [VMEM] * len(args),
        out_specs=jax.tree.map(lambda _: VMEM, out_shape),
        scratch_shapes=list(scratch),
        compiler_params=PARAMS,
        name=name,
    )(*args)


def f32(*shape):
    return jax.ShapeDtypeStruct(shape, jnp.float32)


def load(pairs, sem):
    copies = [pltpu.make_async_copy(a, b, sem.at[i]) for i, (a, b) in enumerate(pairs)]
    for copy in copies:
        copy.start()
    for copy in copies:
        copy.wait()


def pack_kernel(order_in, pose_in, latents_in, out_ref, order_ref, pose_ref, latents_ref, sem):
    load([(order_in, order_ref), (pose_in, pose_ref), (latents_in, latents_ref)], sem)
    k_modes = latents_ref.shape[1]
    lane = lax.broadcasted_iota(jnp.int32, (1, 128), 1)
    diag = lax.broadcasted_iota(jnp.int32, (k_modes, k_modes), 0) == lax.broadcasted_iota(
        jnp.int32, (k_modes, k_modes), 1
    )
    latent = jnp.zeros((k_modes, 128), jnp.float32)
    pose = jnp.zeros((1, 128), jnp.int32)
    turn = jnp.zeros((1, 128), jnp.int32)
    for s in range(STEPS):
        o = order_ref[s]
        n = pose_ref[o]
        row = latents_ref[pl.ds(o, 1), :]
        col = jnp.sum(
            jnp.where(diag, jnp.broadcast_to(row, diag.shape), 0.0), axis=1, keepdims=True
        )
        latent = jnp.where(lane == s, col, latent)
        pose = jnp.where(lane == s, n, pose)
        turn = jnp.where(lane == s, lax.rem(n * 55, 144), turn)
    cb = 1.0 - (2 * pose + 1).astype(jnp.float32) / NROT
    sb = jnp.sqrt(1.0 - cb * cb)
    alpha = turn.astype(jnp.float32) * (2.0 * math.pi / 144.0)
    gamma = (pose & 7).astype(jnp.float32) * (math.pi / 4.0)
    ca, sa = jnp.cos(alpha), jnp.sin(alpha)
    cg, sg = jnp.cos(gamma), jnp.sin(gamma)
    rows = [
        ca * cb * cg - sa * sg,
        -ca * cb * sg - sa * cg,
        ca * sb,
        sa * cb * cg + ca * sg,
        -sa * cb * sg + ca * cg,
        sa * sb,
    ]
    out_ref[0:k_modes, :] = latent
    for i, row in enumerate(rows):
        out_ref[k_modes + i : k_modes + i + 1, :] = row
    out_ref[k_modes + 6 :, :] = jnp.zeros((2, 128), jnp.float32)


def own_kernel(base_in, modes_in, base_ref, modes_ref, sem):
    own = base_ref.shape[1]
    start = pl.multiple_of(lax.axis_index("img") * own, own)
    load([(base_in.at[:, pl.ds(start, own)], base_ref), (modes_in, modes_ref)], sem)


def prepare_kernel(
    order_in, observed_in, amp_in, wid_in, par_ref, obs_ref, order_ref, observed_ref, amp_ref,
    wid_ref, sem,
):
    n_img, _, sub, lanes = par_ref.shape
    me = lax.axis_index("img")
    load(
        [
            (order_in, order_ref),
            (observed_in, observed_ref),
            (amp_in, amp_ref),
            (wid_in, wid_ref),
        ],
        sem,
    )
    for s in range(STEPS):
        obs_ref[s] = observed_ref[order_ref[s]].astype(jnp.float32)
    for t in range(n_img):
        for j in range(sub):
            at = pl.multiple_of(((me ^ t) * sub + j) * lanes, lanes)
            w = wid_ref[pl.ds(at, lanes)].reshape(1, lanes)
            inv = 1.0 / (w * w)
            par_ref[t, 0, j : j + 1, :] = (-0.5 * LOG2E) * inv
            par_ref[t, 1, j : j + 1, :] = amp_ref[pl.ds(at, lanes)].reshape(1, lanes)
            par_ref[t, 2, j : j + 1, :] = inv


def project_kernel(*refs, n_img, center):
    pk = refs[:n_img][::-1]
    base_ref, modes_ref = refs[n_img : n_img + 2]
    outs = refs[n_img + 2 :]
    _, k_modes, own = modes_ref.shape
    lanes = own // SUB
    base = [base_ref[c : c + 1, :] for c in range(3)]
    for s in range(STEPS):
        for t in range(n_img):
            col = jnp.broadcast_to(pk[t][0:k_modes, s : s + 1], (k_modes, own))
            pos = [
                base[c] + jnp.sum(col * modes_ref[c], axis=0, keepdims=True) for c in range(3)
            ]
            for r in range(2):
                o = k_modes + 3 * r
                row = (
                    pk[t][o : o + 1, s : s + 1] * pos[0]
                    + pk[t][o + 1 : o + 2, s : s + 1] * pos[1]
                    + pk[t][o + 2 : o + 3, s : s + 1] * pos[2]
                    + center
                )
                for j in range(SUB):
                    outs[t][s, r, j : j + 1, :] = row[:, j * lanes : (j + 1) * lanes]


def spread_kernel(*refs, n_img, k_modes):
    pk = refs[:n_img][::-1]
    z_ref, r_ref, c_ref = refs[n_img:]
    lanes = z_ref.shape[3]
    for s in range(STEPS):
        for t in range(n_img):
            z_ref[s, t] = jnp.broadcast_to(pk[t][0:k_modes, s : s + 1], (k_modes, lanes))
            r_ref[s, t] = jnp.broadcast_to(pk[t][k_modes : k_modes + 8, s : s + 1], (8, lanes))
    for s in range(STEPS - 1):
        for t in range(n_img):
            zz = jnp.sum(z_ref[s + 1, 0] * z_ref[s, t], axis=0, keepdims=True)
            for r in range(2):
                for r2 in range(2):
                    d = None
                    for c in range(3):
                        e = (
                            r_ref[s + 1, 0, 3 * r + c : 3 * r + c + 1]
                            * r_ref[s, t, 3 * r2 + c : 3 * r2 + c + 1]
                        )
                        d = e if d is None else d + e
                    i = 2 * r + r2
                    c_ref[s, t, i : i + 1] = zz * d


def step_length(s_refs, entries):
    total = s_refs[0][...]
    for ref in s_refs[1:]:
        total = total + ref[...]
    total = jnp.sum(jnp.sum(total, axis=0, keepdims=True), axis=1, keepdims=True)
    return step_size / jnp.sqrt(total / entries + tiny_eps)


def forward_kernel(*refs, n_img, outer, entries, rows, nz):
    p_refs = refs[:n_img][::-1]
    pos = n_img
    if outer:
        q_ref = refs[pos]
        s_refs = refs[pos + 1 : pos + 1 + nz]
        pos += 1 + nz
    par_ref, obs_ref, keep_ref, send_ref, proj_ref, u_ref, v_ref, acc_ref, pix_ref = refs[pos:]
    pix, lanes = pix_ref.shape
    place = lax.axis_index("gauss")
    core = place % 2
    if outer:
        alpha = step_length(s_refs, entries)
    for t in range(n_img):
        p = p_refs[t][outer]
        if outer:
            p = p - alpha * q_ref[t]
        proj_ref[t] = p
    pix_ref[...] = lax.broadcasted_iota(jnp.int32, (pix, lanes), 0).astype(jnp.float32)
    acc_ref[...] = jnp.zeros_like(acc_ref)

    def slot(t, carry):
        total = None
        for j in range(SUB):
            c = par_ref[t, 0, j : j + 1, :]
            a = par_ref[t, 1, j : j + 1, :]
            du = pix_ref[...] - proj_ref[t, 0, j : j + 1, :]
            dv = pix_ref[...] - proj_ref[t, 1, j : j + 1, :]
            u = jnp.exp2(du * du * c).astype(jnp.bfloat16)
            v = (a * jnp.exp2(dv * dv * c)).astype(jnp.bfloat16)
            u_ref[t, j] = u
            v_ref[t, j] = v
            term = lax.dot_general(
                u, v, (((1,), (1,)), ((), ())), preferred_element_type=jnp.float32
            )
            total = term if total is None else total + term
        acc_ref[...] += total
        return carry

    lax.fori_loop(0, n_img, slot, 0)
    for z in range(nz):
        keep_ref[z] = acc_ref[pl.ds(pl.multiple_of((2 * z + core) * rows, 8), rows), :]
        send_ref[z] = acc_ref[pl.ds(pl.multiple_of((2 * z + 1 - core) * rows, 8), rows), :]
    keep_ref[place // 2] -= obs_ref[outer]


def moment(profile, weighted, mean):
    pix, lanes = weighted.shape
    n = pix // SUB
    run = None
    runs = None
    for i in range(n):
        x = profile[SUB * i : SUB * (i + 1)].astype(jnp.float32) * weighted[SUB * i : SUB * (i + 1)]
        run = x if run is None else run + x
        if i + 1 < n:
            runs = run if runs is None else runs + run
    sub = lax.broadcasted_iota(jnp.int32, (SUB, lanes), 0).astype(jnp.float32)
    at = sub - mean + float(SUB * (n - 1))
    return jnp.sum(run * at - float(SUB) * runs, axis=0, keepdims=True)


def backward_kernel(
    own_ref, other_ref, proj_ref, par_ref, u_ref, v_ref, out_ref, res_ref, rest_ref,
    *, n_img, rows, nz
):
    core = lax.axis_index("gauss") % 2
    for z in range(nz):
        res_ref[pl.ds(pl.multiple_of((2 * z + core) * rows, 16), rows), :] = own_ref[z]
        res_ref[pl.ds(pl.multiple_of((2 * z + 1 - core) * rows, 16), rows), :] = other_ref[z]
    rest_ref[...] = res_ref[...].astype(jnp.float32).T.astype(jnp.bfloat16)

    def slot(t, carry):
        for j in range(SUB):
            inv = par_ref[t, 2, j : j + 1, :]
            u = u_ref[t, j]
            v = v_ref[t, j]
            wu = jnp.dot(res_ref[...], v, preferred_element_type=jnp.float32)
            wv = jnp.dot(rest_ref[...], u, preferred_element_type=jnp.float32)
            mu = proj_ref[t, 0, j : j + 1, :]
            mv = proj_ref[t, 1, j : j + 1, :]
            out_ref[t, 0, j : j + 1, :] = inv * moment(u, wu, mu)
            out_ref[t, 1, j : j + 1, :] = inv * moment(v, wv, mv)
        return carry

    lax.fori_loop(0, n_img, slot, 0, unroll=2)


def shifts_of(r_ref, s, t, gu, gv, c):
    return r_ref[s, t, c : c + 1] * gu + r_ref[s, t, 3 + c : 4 + c] * gv


def squares_kernel(*refs, n_img, outer, with_q):
    z_ref, r_ref, c_ref = refs[:3]
    g = refs[3 : 3 + n_img][::-1]
    outs = refs[3 + n_img :]
    s_ref, shift_ref = outs[0], outs[-1]
    k_modes, lanes = z_ref.shape[2:]
    z = [z_ref[outer, t] for t in range(n_img)]
    squares = jnp.zeros((k_modes, lanes), jnp.float32)
    for t0 in range(n_img):
        gu = [g[t][t0 ^ t, 0] for t in range(n_img)]
        gv = [g[t][t0 ^ t, 1] for t in range(n_img)]
        for r in range(2 if with_q else 0):
            q = None
            for t in range(n_img):
                e = (
                    c_ref[outer, t, 2 * r : 2 * r + 1] * gu[t]
                    + c_ref[outer, t, 2 * r + 1 : 2 * r + 2] * gv[t]
                )
                q = e if q is None else q + e
            outs[1][t0, r] = q
        for c in range(3):
            for t in range(n_img):
                shift_ref[t0, c, t] = shifts_of(r_ref, outer, t, gu[t], gv[t], c)
    for t0 in range(n_img):
        for c in range(3):
            for j in range(SUB):
                m = None
                for t in range(n_img):
                    e = z[t] * shift_ref[t0, c, t, j : j + 1]
                    m = e if m is None else m + e
                squares = squares + m * m
    part = None
    for k in range(0, k_modes, SUB):
        for i in range(0, lanes, 128):
            e = squares[k : k + SUB, i : i + 128]
            part = e if part is None else part + e
    s_ref[...] = part


def update_kernel(*refs, n_img, nz, entries):
    z_ref, r_ref = refs[:2]
    pos = 2
    g = [refs[pos + s * n_img : pos + (s + 1) * n_img][::-1] for s in range(STEPS)]
    pos += STEPS * n_img
    s_refs = [refs[pos + s * nz : pos + (s + 1) * nz] for s in range(STEPS)]
    modes_ref, out_ref, shift_ref = refs[pos + STEPS * nz :]
    lanes = z_ref.shape[3]
    for s in range(STEPS):
        alpha = step_length(s_refs[s], entries)
        for t in range(n_img):
            gu = alpha * g[s][t][t, 0]
            gv = alpha * g[s][t][t, 1]
            for c in range(3):
                shift_ref[s, t, c] = shifts_of(r_ref, s, t, gu, gv, c)
    for c in range(3):
        for j in range(SUB):
            m = modes_ref[c, :, j * lanes : (j + 1) * lanes]
            for s in range(STEPS):
                for t in range(n_img):
                    m = m - z_ref[s, t] * shift_ref[s, t, c, j : j + 1]
            out_ref[c, :, j * lanes : (j + 1) * lanes] = m


def body(
    observed, pose_index, batch_order, latents, base_positions, amplitudes, widths, deform_modes
):
    n_img = lax.axis_size("img")
    n_gauss = lax.axis_size("gauss")
    zplace = lax.axis_index("gauss") // 2
    nz = n_gauss // 2
    _, rows, pix = observed.shape
    k_modes, _, own = deform_modes.shape
    entries = 3 * k_modes * base_positions.shape[1] * n_gauss
    lanes = own // SUB
    modes = jnp.transpose(deform_modes, (1, 0, 2))
    part_fn = functools.partial

    pack = call(
        pack_kernel, "pack", f32(k_modes + 8, 128), (batch_order, pose_index, latents), [HBM] * 3,
        [pltpu.SMEM(batch_order.shape, jnp.int32), pltpu.SMEM(pose_index.shape, jnp.int32),
         pltpu.VMEM(latents.shape, jnp.float32), pltpu.SemaphoreType.DMA((3,))],
    )
    pk = spread_out([pack] * n_img, "img")
    base, modes = call(
        own_kernel, "own", [f32(3, own), f32(3, k_modes, own)], (base_positions, modes), [HBM] * 2,
        [pltpu.SemaphoreType.DMA((2,))],
    )
    par, obs = call(
        prepare_kernel, "prepare", [f32(n_img, 3, SUB, lanes), f32(STEPS, rows, pix)],
        (batch_order, observed, amplitudes, widths), [HBM] * 4,
        [pltpu.SMEM(batch_order.shape, jnp.int32), pltpu.VMEM(observed.shape, observed.dtype),
         pltpu.VMEM(amplitudes.shape, jnp.float32), pltpu.VMEM(widths.shape, jnp.float32),
         pltpu.SemaphoreType.DMA((4,))],
    )
    proj = call(
        part_fn(project_kernel, n_img=n_img, center=(pix - 1) * 0.5), "project",
        [f32(STEPS, 2, SUB, lanes)] * n_img, (*pk[::-1], base, modes),
    )
    proj = spread_out(proj, "img")
    zs, rs, cs = call(
        part_fn(spread_kernel, n_img=n_img, k_modes=k_modes), "spread",
        [f32(STEPS, n_img, k_modes, lanes), f32(STEPS, n_img, 8, lanes),
         f32(STEPS - 1, n_img, 8, lanes)],
        pk[::-1],
    )

    extra = []
    grads, sums = [], []
    half_shape = f32(nz, rows, pix)
    per_shard = f32(n_img, 2, SUB, lanes)
    profile = jax.ShapeDtypeStruct((n_img, SUB, pix, lanes), jnp.bfloat16)
    for outer in range(STEPS):
        keep, send, here, u, v = call(
            part_fn(forward_kernel, n_img=n_img, outer=outer, entries=entries, rows=rows, nz=nz),
            "forward", [half_shape, half_shape, per_shard, profile, profile], (*proj[::-1], *extra, par, obs),
            scratch=[pltpu.VMEM((pix, pix), jnp.float32), pltpu.VMEM((pix, lanes), jnp.float32)],
        )
        part = keep + exchange(send, "gauss", 1)
        bit = 2
        while bit < n_gauss:
            part = part + exchange(part.astype(jnp.bfloat16), "gauss", bit).astype(jnp.float32)
            bit *= 2
        half = part.astype(jnp.bfloat16)
        other = exchange(half, "gauss", 1)
        g = call(
            part_fn(backward_kernel, n_img=n_img, rows=rows, nz=nz), "backward", per_shard,
            (half, other, here, par, u, v),
            scratch=[pltpu.VMEM((pix, pix), jnp.bfloat16)] * 2,
        )
        g = spread_out([g] * n_img, "img")
        more = outer + 1 < STEPS
        out = call(
            part_fn(squares_kernel, n_img=n_img, outer=outer, with_q=more), "squares",
            [f32(SUB, 128)] + [per_shard] * more, (zs, rs, cs, *g[::-1]),
            scratch=[pltpu.VMEM((n_img, 3, n_img, SUB, lanes), jnp.float32)],
        )
        s_chip = out[0] + exchange(out[0], "gauss", 1)
        s_all = spread_out([s_chip] * nz, "gauss", 2)
        extra = [out[-1], *s_all[::-1]]
        grads.extend(g[::-1])
        sums.extend(s_all[::-1])
    final_rows = lax.dynamic_index_in_dim(part, zplace, 0, keepdims=False)
    new = call(
        part_fn(update_kernel, n_img=n_img, nz=nz, entries=entries), "update", f32(*modes.shape),
        (zs, rs, *grads, *sums, modes),
        scratch=[pltpu.VMEM((STEPS, n_img, 3, SUB, lanes), jnp.float32)],
    )
    return (final_rows[None], jnp.transpose(new, (1, 0, 2)))


def solution(mesh):
    return jax.shard_map(
        body,
        mesh=mesh,
        in_specs=(
            P("img", "gauss", None),
            P("img"),
            P("img"),
            P("img", None),
            P(None, "gauss"),
            P("gauss"),
            P("gauss"),
            P(None, None, ("gauss", "img")),
        ),
        out_specs=(P("img", "gauss", None), P(None, None, ("gauss", "img"))),
        check_vma=False,
    )
```

```python
import functools
import math

import jax
import jax.numpy as jnp
from jax import lax
from jax.experimental import pallas as pl
from jax.experimental.pallas import tpu as pltpu
from jax.sharding import PartitionSpec as P

NROT = 4096
STEPS = 2
SUB = 8

step_size = 0.5
tiny_eps = 1e-06
LOG2E = 1.4426950408889634


SMEM = pl.BlockSpec(memory_space=pltpu.SMEM)
VMEM = pl.BlockSpec(memory_space=pltpu.VMEM)
HBM = pl.BlockSpec(memory_space=pltpu.HBM)
PARAMS = pltpu.CompilerParams(vmem_limit_bytes=16 << 20)


def xor_pairs(n, s):
    return [(i, i ^ s) for i in range(n)]


def exchange(x, axis, s):
    return lax.ppermute(x, axis, xor_pairs(lax.axis_size(axis), s))


def spread_out(parts, axis, unit=1):
    far_first = range(len(parts) - 1, 0, -1)
    got = {t: exchange(parts[t], axis, t * unit) for t in far_first}
    return [parts[0]] + [got[t] for t in range(1, len(parts))]


def call(kernel, name, out_shape, args, in_specs=None, scratch=(), params=PARAMS):
    return pl.pallas_call(
        kernel,
        out_shape=out_shape,
        in_specs=in_specs or [VMEM] * len(args),
        out_specs=jax.tree.map(lambda _: VMEM, out_shape),
        scratch_shapes=list(scratch),
        compiler_params=params,
        name=name,
    )(*args)


def f32(*shape):
    return jax.ShapeDtypeStruct(shape, jnp.float32)


def load(pairs, sem):
    copies = [pltpu.make_async_copy(a, b, sem.at[i]) for i, (a, b) in enumerate(pairs)]
    for copy in copies:
        copy.start()
    for copy in copies:
        copy.wait()


def pack_kernel(order_in, pose_in, latents_in, out_ref, order_ref, pose_ref, latents_ref, sem):
    load([(order_in, order_ref), (pose_in, pose_ref), (latents_in, latents_ref)], sem)
    k_modes = latents_ref.shape[1]
    lane = lax.broadcasted_iota(jnp.int32, (1, 128), 1)
    diag = lax.broadcasted_iota(jnp.int32, (k_modes, k_modes), 0) == lax.broadcasted_iota(
        jnp.int32, (k_modes, k_modes), 1
    )
    latent = jnp.zeros((k_modes, 128), jnp.float32)
    pose = jnp.zeros((1, 128), jnp.int32)
    turn = jnp.zeros((1, 128), jnp.int32)
    order = jnp.zeros((1, 128), jnp.int32)
    for s in range(STEPS):
        o = order_ref[s]
        n = pose_ref[o]
        row = latents_ref[pl.ds(o, 1), :]
        col = jnp.sum(
            jnp.where(diag, jnp.broadcast_to(row, diag.shape), 0.0), axis=1, keepdims=True
        )
        latent = jnp.where(lane == s, col, latent)
        pose = jnp.where(lane == s, n, pose)
        order = jnp.where(lane == s, o, order)
        turn = jnp.where(lane == s, lax.rem(n * 55, 144), turn)
    cb = 1.0 - (2 * pose + 1).astype(jnp.float32) / NROT
    sb = jnp.sqrt(1.0 - cb * cb)
    alpha = turn.astype(jnp.float32) * (2.0 * math.pi / 144.0)
    gamma = (pose & 7).astype(jnp.float32) * (math.pi / 4.0)
    ca, sa = jnp.cos(alpha), jnp.sin(alpha)
    cg, sg = jnp.cos(gamma), jnp.sin(gamma)
    rows = [
        ca * cb * cg - sa * sg,
        -ca * cb * sg - sa * cg,
        ca * sb,
        sa * cb * cg + ca * sg,
        -sa * cb * sg + ca * cg,
        sa * sb,
        order.astype(jnp.float32),
    ]
    out_ref[0:k_modes, :] = latent
    for i, row in enumerate(rows):
        out_ref[k_modes + i : k_modes + i + 1, :] = row
    out_ref[k_modes + 7 :, :] = jnp.zeros((1, 128), jnp.float32)


def own_kernel(base_in, modes_in, base_ref, modes_ref, dense_base_ref, dense_ref, sem):
    _, k_modes, own = modes_ref.shape
    lanes = own // SUB
    start = pl.multiple_of(lax.axis_index("img") * own, own)
    load([(base_in.at[:, pl.ds(start, own)], base_ref), (modes_in, modes_ref)], sem)
    for c in range(3):
        for j in range(SUB):
            at = slice(j * lanes, (j + 1) * lanes)
            dense_base_ref[c, j : j + 1, :] = base_ref[c : c + 1, at]
            for i in range(lanes // 128):
                part = slice(j * lanes + 128 * i, j * lanes + 128 * (i + 1))
                dense_ref[c, i, pl.ds(j, k_modes, stride=SUB), :] = modes_ref[c, :, part]


def prepare_kernel(pack_ref, observed_ref, amp_ref, wid_ref, par_ref, obs_ref):
    n_img, _, sub, lanes = par_ref.shape
    me = lax.axis_index("img")
    at = pack_ref.shape[0] - 2
    for s in range(STEPS):
        order = jnp.broadcast_to(pack_ref[at : at + 1, s : s + 1], (1, obs_ref.shape[2]))
        picked = observed_ref[0].astype(jnp.float32)
        for o in range(1, observed_ref.shape[0]):
            picked = jnp.where(order == float(o), observed_ref[o].astype(jnp.float32), picked)
        obs_ref[s] = picked
    for t in range(n_img):
        for j in range(sub):
            at = pl.multiple_of(((me ^ t) * sub + j) * lanes, lanes)
            w = wid_ref[pl.ds(at, lanes)].reshape(1, lanes)
            inv = 1.0 / (w * w)
            par_ref[t, 0, j : j + 1, :] = (-0.5 * LOG2E) * inv
            par_ref[t, 1, j : j + 1, :] = amp_ref[pl.ds(at, lanes)].reshape(1, lanes)
            par_ref[t, 2, j : j + 1, :] = inv


def project_kernel(z_ref, r_ref, base_ref, modes_ref, *outs, center):
    n_img, k_modes, lanes = z_ref.shape[1:]
    n_img = len(outs)
    outs = outs[::-1]
    for s in range(STEPS):
        for t in range(n_img):
            for i in range(lanes // 128):
                at = slice(128 * i, 128 * (i + 1))
                pos = []
                for c in range(3):
                    acc = None
                    for k in range(k_modes):
                        e = z_ref[s, t, k : k + 1, at] * modes_ref[c, i, SUB * k : SUB * (k + 1), :]
                        acc = e if acc is None else acc + e
                    pos.append(base_ref[c, :, at] + acc)
                for r in range(2):
                    outs[t][s, r, :, at] = (
                        r_ref[s, t, 3 * r : 3 * r + 1, at] * pos[0]
                        + r_ref[s, t, 3 * r + 1 : 3 * r + 2, at] * pos[1]
                        + r_ref[s, t, 3 * r + 2 : 3 * r + 3, at] * pos[2]
                        + center
                    )


def spread_kernel(*refs, n_img, k_modes):
    pk = refs[:n_img][::-1]
    z_ref, r_ref, c_ref = refs[n_img:]
    lanes = z_ref.shape[3]
    for s in range(STEPS):
        for t in range(n_img):
            z_ref[s, t] = jnp.broadcast_to(pk[t][0:k_modes, s : s + 1], (k_modes, lanes))
            r_ref[s, t] = jnp.broadcast_to(pk[t][k_modes : k_modes + 8, s : s + 1], (8, lanes))
    for s in range(STEPS - 1):
        for t in range(n_img):
            zz = jnp.sum(z_ref[s + 1, 0] * z_ref[s, t], axis=0, keepdims=True)
            for r in range(2):
                for r2 in range(2):
                    d = None
                    for c in range(3):
                        e = (
                            r_ref[s + 1, 0, 3 * r + c : 3 * r + c + 1]
                            * r_ref[s, t, 3 * r2 + c : 3 * r2 + c + 1]
                        )
                        d = e if d is None else d + e
                    i = 2 * r + r2
                    c_ref[s, t, i : i + 1] = zz * d


def step_length(s_refs, entries):
    total = s_refs[0][...]
    for ref in s_refs[1:]:
        total = total + ref[...]
    total = jnp.sum(jnp.sum(total, axis=0, keepdims=True), axis=1, keepdims=True)
    return step_size / jnp.sqrt(total / entries + tiny_eps)


def forward_kernel(*refs, n_img, outer, entries, rows, nz):
    p_refs = refs[:n_img][::-1]
    pos = n_img
    if outer:
        q_ref = refs[pos]
        s_refs = refs[pos + 1 : pos + 1 + nz]
        pos += 1 + nz
    par_ref, obs_ref, keep_ref, send_ref, proj_ref, u_ref, v_ref, acc_ref, pix_ref = refs[pos:]
    pix, lanes = pix_ref.shape
    place = lax.axis_index("gauss")
    core = place % 2
    if outer:
        alpha = step_length(s_refs, entries)
    for t in range(n_img):
        p = p_refs[t][outer]
        if outer:
            p = p - alpha * q_ref[t]
        proj_ref[t] = p
    pix_ref[...] = lax.broadcasted_iota(jnp.int32, (pix, lanes), 0).astype(jnp.float32)
    acc_ref[...] = jnp.zeros_like(acc_ref)

    def slot(t, carry):
        total = None
        for j in range(SUB):
            c = par_ref[t, 0, j : j + 1, :]
            a = par_ref[t, 1, j : j + 1, :]
            du = pix_ref[...] - proj_ref[t, 0, j : j + 1, :]
            dv = pix_ref[...] - proj_ref[t, 1, j : j + 1, :]
            u = jnp.exp2(du * du * c).astype(jnp.bfloat16)
            v = (a * jnp.exp2(dv * dv * c)).astype(jnp.bfloat16)
            u_ref[t, j] = u
            v_ref[t, j] = v
            term = lax.dot_general(
                u, v, (((1,), (1,)), ((), ())), preferred_element_type=jnp.float32
            )
            total = term if total is None else total + term
        acc_ref[...] += total
        return carry

    lax.fori_loop(0, n_img, slot, 0)
    for z in range(nz):
        keep_ref[z] = acc_ref[pl.ds(pl.multiple_of((2 * z + core) * rows, 8), rows), :]
        send_ref[z] = acc_ref[pl.ds(pl.multiple_of((2 * z + 1 - core) * rows, 8), rows), :]
    keep_ref[place // 2] -= obs_ref[outer]


def moment(profile, weighted, mean):
    pix, lanes = weighted.shape
    n = pix // SUB
    run = None
    runs = None
    for i in range(n):
        x = profile[SUB * i : SUB * (i + 1)].astype(jnp.float32) * weighted[SUB * i : SUB * (i + 1)]
        run = x if run is None else run + x
        if i + 1 < n:
            runs = run if runs is None else runs + run
    sub = lax.broadcasted_iota(jnp.int32, (SUB, lanes), 0).astype(jnp.float32)
    at = sub - mean + float(SUB * (n - 1))
    return jnp.sum(run * at - float(SUB) * runs, axis=0, keepdims=True)


def backward_kernel(
    own_ref, other_ref, proj_ref, par_ref, u_ref, v_ref, out_ref, res_ref, rest_ref,
    *, n_img, rows, nz
):
    core = lax.axis_index("gauss") % 2
    for z in range(nz):
        res_ref[pl.ds(pl.multiple_of((2 * z + core) * rows, 16), rows), :] = own_ref[z]
        res_ref[pl.ds(pl.multiple_of((2 * z + 1 - core) * rows, 16), rows), :] = other_ref[z]
    rest_ref[...] = res_ref[...].astype(jnp.float32).T.astype(jnp.bfloat16)

    def slot(t, carry):
        for j in range(SUB):
            inv = par_ref[t, 2, j : j + 1, :]
            u = u_ref[t, j]
            v = v_ref[t, j]
            wu = jnp.dot(res_ref[...], v, preferred_element_type=jnp.float32)
            wv = jnp.dot(rest_ref[...], u, preferred_element_type=jnp.float32)
            mu = proj_ref[t, 0, j : j + 1, :]
            mv = proj_ref[t, 1, j : j + 1, :]
            out_ref[t, 0, j : j + 1, :] = inv * moment(u, wu, mu)
            out_ref[t, 1, j : j + 1, :] = inv * moment(v, wv, mv)
        return carry

    lax.fori_loop(0, n_img, slot, 0, unroll=2)


def shifts_of(r_ref, s, t, gu, gv, c):
    return r_ref[s, t, c : c + 1] * gu + r_ref[s, t, 3 + c : 4 + c] * gv


def squares_kernel(*refs, n_img, outer, with_q):
    z_ref, r_ref, c_ref = refs[:3]
    g = refs[3 : 3 + n_img][::-1]
    outs = refs[3 + n_img :]
    s_ref, shift_ref = outs[0], outs[-1]
    k_modes, lanes = z_ref.shape[2:]
    z = [z_ref[outer, t] for t in range(n_img)]
    squares = jnp.zeros((k_modes, lanes), jnp.float32)
    for t0 in range(n_img):
        gu = [g[t][t0 ^ t, 0].astype(jnp.float32) for t in range(n_img)]
        gv = [g[t][t0 ^ t, 1].astype(jnp.float32) for t in range(n_img)]
        for r in range(2 if with_q else 0):
            q = None
            for t in range(n_img):
                e = (
                    c_ref[outer, t, 2 * r : 2 * r + 1] * gu[t]
                    + c_ref[outer, t, 2 * r + 1 : 2 * r + 2] * gv[t]
                )
                q = e if q is None else q + e
            outs[1][t0, r] = q
        for c in range(3):
            for t in range(n_img):
                shift_ref[t0, c, t] = shifts_of(r_ref, outer, t, gu[t], gv[t], c)
    for t0 in range(n_img):
        for c in range(3):
            for j in range(SUB):
                m = None
                for t in range(n_img):
                    e = z[t] * shift_ref[t0, c, t, j : j + 1]
                    m = e if m is None else m + e
                squares = squares + m * m
    part = None
    for k in range(0, k_modes, SUB):
        for i in range(0, lanes, 128):
            e = squares[k : k + SUB, i : i + 128]
            part = e if part is None else part + e
    s_ref[...] = part


def update_kernel(*refs, n_img, nz, entries):
    z_ref, r_ref = refs[:2]
    pos = 2
    g = [refs[pos + s * n_img : pos + (s + 1) * n_img][::-1] for s in range(STEPS)]
    pos += STEPS * n_img
    s_refs = [refs[pos + s * nz : pos + (s + 1) * nz] for s in range(STEPS)]
    modes_ref, out_ref, shift_ref = refs[pos + STEPS * nz :]
    lanes = z_ref.shape[3]
    for s in range(STEPS):
        alpha = step_length(s_refs[s], entries)
        for t in range(n_img):
            gu = alpha * g[s][t][t, 0].astype(jnp.float32)
            gv = alpha * g[s][t][t, 1].astype(jnp.float32)
            for c in range(3):
                shift_ref[s, t, c] = shifts_of(r_ref, s, t, gu, gv, c)
    for c in range(3):
        for j in range(SUB):
            m = modes_ref[c, :, j * lanes : (j + 1) * lanes]
            for s in range(STEPS):
                for t in range(n_img):
                    m = m - z_ref[s, t] * shift_ref[s, t, c, j : j + 1]
            out_ref[c, :, j * lanes : (j + 1) * lanes] = m


def body(
    observed, pose_index, batch_order, latents, base_positions, amplitudes, widths, deform_modes
):
    n_img = lax.axis_size("img")
    n_gauss = lax.axis_size("gauss")
    zplace = lax.axis_index("gauss") // 2
    nz = n_gauss // 2
    _, rows, pix = observed.shape
    k_modes, _, own = deform_modes.shape
    entries = 3 * k_modes * base_positions.shape[1] * n_gauss
    lanes = own // SUB
    modes = jnp.transpose(deform_modes, (1, 0, 2))
    part_fn = functools.partial

    pack = call(
        pack_kernel, "pack", f32(k_modes + 8, 128), (batch_order, pose_index, latents), [HBM] * 3,
        [pltpu.SMEM(batch_order.shape, jnp.int32), pltpu.SMEM(pose_index.shape, jnp.int32),
         pltpu.VMEM(latents.shape, jnp.float32), pltpu.SemaphoreType.DMA((3,))],
        pltpu.CompilerParams(vmem_limit_bytes=67018752),
    )
    pk = spread_out([pack] * n_img, "img")
    own_base, modes, dense_base, dense = call(
        own_kernel, "own",
        [f32(3, own), f32(3, k_modes, own), f32(3, SUB, lanes),
         f32(3, lanes // 128, k_modes * SUB, 128)],
        (base_positions, modes), [HBM] * 2, [pltpu.SemaphoreType.DMA((2,))],
    )
    par, obs = call(
        prepare_kernel, "prepare", [f32(n_img, 3, SUB, lanes), f32(STEPS, rows, pix)],
        (pack, observed, amplitudes, widths),
    )
    zs, rs, cs = call(
        part_fn(spread_kernel, n_img=n_img, k_modes=k_modes), "spread",
        [f32(STEPS, n_img, k_modes, lanes), f32(STEPS, n_img, 8, lanes),
         f32(STEPS - 1, n_img, 8, lanes)],
        pk[::-1],
    )
    proj = call(
        part_fn(project_kernel, center=(pix - 1) * 0.5), "project",
        [f32(STEPS, 2, SUB, lanes)] * n_img, (zs, rs, dense_base, dense),
    )[::-1]
    proj = spread_out(proj, "img")

    extra = []
    grads, sums = [], []
    half_shape = f32(nz, rows, pix)
    per_shard = f32(n_img, 2, SUB, lanes)
    profile = jax.ShapeDtypeStruct((n_img, SUB, pix, lanes), jnp.bfloat16)
    for outer in range(STEPS):
        keep, send, here, u, v = call(
            part_fn(forward_kernel, n_img=n_img, outer=outer, entries=entries, rows=rows, nz=nz),
            "forward", [half_shape, half_shape, per_shard, profile, profile], (*proj[::-1], *extra, par, obs),
            scratch=[pltpu.VMEM((pix, pix), jnp.float32), pltpu.VMEM((pix, lanes), jnp.float32)],
        )
        part = keep + exchange(send, "gauss", 1)
        bit = 2
        while bit < n_gauss:
            part = part + exchange(part.astype(jnp.bfloat16), "gauss", bit).astype(jnp.float32)
            bit *= 2
        half = part.astype(jnp.bfloat16)
        other = exchange(half, "gauss", 1)
        g = call(
            part_fn(backward_kernel, n_img=n_img, rows=rows, nz=nz), "backward", per_shard,
            (half, other, here, par, u, v),
            scratch=[pltpu.VMEM((pix, pix), jnp.bfloat16)] * 2,
        )
        g = spread_out([g] + [g.astype(jnp.bfloat16)] * (n_img - 1), "img")
        more = outer + 1 < STEPS
        out = call(
            part_fn(squares_kernel, n_img=n_img, outer=outer, with_q=more), "squares",
            [f32(SUB, 128)] + [per_shard] * more, (zs, rs, cs, *g[::-1]),
            scratch=[pltpu.VMEM((n_img, 3, n_img, SUB, lanes), jnp.float32)],
        )
        s_chip = out[0] + exchange(out[0], "gauss", 1)
        s_all = spread_out([s_chip] * nz, "gauss", 2)
        extra = [out[-1], *s_all[::-1]]
        grads.extend(g[::-1])
        sums.extend(s_all[::-1])
    final_rows = lax.dynamic_index_in_dim(part, zplace, 0, keepdims=False)
    new = call(
        part_fn(update_kernel, n_img=n_img, nz=nz, entries=entries), "update", f32(*modes.shape),
        (zs, rs, *grads, *sums, modes),
        scratch=[pltpu.VMEM((STEPS, n_img, 3, SUB, lanes), jnp.float32)],
    )
    return (final_rows[None], jnp.transpose(new, (1, 0, 2)))


def solution(mesh):
    return jax.shard_map(
        body,
        mesh=mesh,
        in_specs=(
            P("img", "gauss", None),
            P("img"),
            P("img"),
            P("img", None),
            P(None, "gauss"),
            P("gauss"),
            P("gauss"),
            P(None, None, ("gauss", "img")),
        ),
        out_specs=(P("img", "gauss", None), P(None, None, ("gauss", "img"))),
        check_vma=False,
    )
```

```python
import functools
import math

import jax
import jax.numpy as jnp
from jax import lax
from jax.experimental import pallas as pl
from jax.experimental.pallas import tpu as pltpu
from jax.sharding import PartitionSpec as P

NROT = 4096
STEPS = 2
SUB = 8

step_size = 0.5
tiny_eps = 1e-06
LOG2E = 1.4426950408889634


SMEM = pl.BlockSpec(memory_space=pltpu.SMEM)
VMEM = pl.BlockSpec(memory_space=pltpu.VMEM)
HBM = pl.BlockSpec(memory_space=pltpu.HBM)
PARAMS = pltpu.CompilerParams(vmem_limit_bytes=16 << 20)


def xor_pairs(n, s):
    return [(i, i ^ s) for i in range(n)]


def exchange(x, axis, s):
    return lax.ppermute(x, axis, xor_pairs(lax.axis_size(axis), s))


def spread_out(parts, axis, unit=1):
    far_first = range(len(parts) - 1, 0, -1)
    got = {t: exchange(parts[t], axis, t * unit) for t in far_first}
    return [parts[0]] + [got[t] for t in range(1, len(parts))]


def call(kernel, name, out_shape, args, in_specs=None, scratch=(), params=PARAMS):
    return pl.pallas_call(
        kernel,
        out_shape=out_shape,
        in_specs=in_specs or [VMEM] * len(args),
        out_specs=jax.tree.map(lambda _: VMEM, out_shape),
        scratch_shapes=list(scratch),
        compiler_params=params,
        name=name,
    )(*args)


def f32(*shape):
    return jax.ShapeDtypeStruct(shape, jnp.float32)


def load(pairs, sem):
    copies = [pltpu.make_async_copy(a, b, sem.at[i]) for i, (a, b) in enumerate(pairs)]
    for copy in copies:
        copy.start()
    for copy in copies:
        copy.wait()


def pack_kernel(order_in, pose_in, latents_in, out_ref, order_ref, pose_ref, latents_ref, sem):
    load([(order_in, order_ref), (pose_in, pose_ref), (latents_in, latents_ref)], sem)
    k_modes = latents_ref.shape[1]
    lane = lax.broadcasted_iota(jnp.int32, (1, 128), 1)
    diag = lax.broadcasted_iota(jnp.int32, (k_modes, k_modes), 0) == lax.broadcasted_iota(
        jnp.int32, (k_modes, k_modes), 1
    )
    latent = jnp.zeros((k_modes, 128), jnp.float32)
    pose = jnp.zeros((1, 128), jnp.int32)
    turn = jnp.zeros((1, 128), jnp.int32)
    order = jnp.zeros((1, 128), jnp.int32)
    for s in range(STEPS):
        o = order_ref[s]
        n = pose_ref[o]
        row = latents_ref[pl.ds(o, 1), :]
        col = jnp.sum(
            jnp.where(diag, jnp.broadcast_to(row, diag.shape), 0.0), axis=1, keepdims=True
        )
        latent = jnp.where(lane == s, col, latent)
        pose = jnp.where(lane == s, n, pose)
        order = jnp.where(lane == s, o, order)
        turn = jnp.where(lane == s, lax.rem(n * 55, 144), turn)
    cb = 1.0 - (2 * pose + 1).astype(jnp.float32) / NROT
    sb = jnp.sqrt(1.0 - cb * cb)
    alpha = turn.astype(jnp.float32) * (2.0 * math.pi / 144.0)
    gamma = (pose & 7).astype(jnp.float32) * (math.pi / 4.0)
    ca, sa = jnp.cos(alpha), jnp.sin(alpha)
    cg, sg = jnp.cos(gamma), jnp.sin(gamma)
    rows = [
        ca * cb * cg - sa * sg,
        -ca * cb * sg - sa * cg,
        ca * sb,
        sa * cb * cg + ca * sg,
        -sa * cb * sg + ca * cg,
        sa * sb,
        order.astype(jnp.float32),
    ]
    out_ref[0:k_modes, :] = latent
    for i, row in enumerate(rows):
        out_ref[k_modes + i : k_modes + i + 1, :] = row
    out_ref[k_modes + 7 :, :] = jnp.zeros((1, 128), jnp.float32)


def own_kernel(base_in, modes_in, base_ref, modes_ref, dense_base_ref, dense_ref, sem):
    _, k_modes, own = modes_ref.shape
    lanes = own // SUB
    start = pl.multiple_of(lax.axis_index("img") * own, own)
    load([(base_in.at[:, pl.ds(start, own)], base_ref), (modes_in, modes_ref)], sem)
    for c in range(3):
        for j in range(SUB):
            at = slice(j * lanes, (j + 1) * lanes)
            dense_base_ref[c, j : j + 1, :] = base_ref[c : c + 1, at]
            for i in range(lanes // 128):
                part = slice(j * lanes + 128 * i, j * lanes + 128 * (i + 1))
                dense_ref[c, i, pl.ds(j, k_modes, stride=SUB), :] = modes_ref[c, :, part]


def prepare_kernel(pack_ref, observed_ref, amp_ref, wid_ref, par_ref, obs_ref):
    n_img, _, sub, lanes = par_ref.shape
    me = lax.axis_index("img")
    at = pack_ref.shape[0] - 2
    for s in range(STEPS):
        order = jnp.broadcast_to(pack_ref[at : at + 1, s : s + 1], (1, obs_ref.shape[2]))
        picked = observed_ref[0].astype(jnp.float32)
        for o in range(1, observed_ref.shape[0]):
            picked = jnp.where(order == float(o), observed_ref[o].astype(jnp.float32), picked)
        obs_ref[s] = picked
    for t in range(n_img):
        for j in range(sub):
            at = pl.multiple_of(((me ^ t) * sub + j) * lanes, lanes)
            w = wid_ref[pl.ds(at, lanes)].reshape(1, lanes)
            inv = 1.0 / (w * w)
            par_ref[t, 0, j : j + 1, :] = (-0.5 * LOG2E) * inv
            par_ref[t, 1, j : j + 1, :] = amp_ref[pl.ds(at, lanes)].reshape(1, lanes)
            par_ref[t, 2, j : j + 1, :] = inv


def project_kernel(z_ref, r_ref, base_ref, modes_ref, *outs, center):
    n_img, k_modes, lanes = z_ref.shape[1:]
    n_img = len(outs)
    outs = outs[::-1]
    for s in range(STEPS):
        for t in range(n_img):
            for i in range(lanes // 128):
                at = slice(128 * i, 128 * (i + 1))
                pos = []
                for c in range(3):
                    acc = None
                    for k in range(k_modes):
                        e = z_ref[s, t, k : k + 1, at] * modes_ref[c, i, SUB * k : SUB * (k + 1), :]
                        acc = e if acc is None else acc + e
                    pos.append(base_ref[c, :, at] + acc)
                for r in range(2):
                    outs[t][s, r, :, at] = (
                        r_ref[s, t, 3 * r : 3 * r + 1, at] * pos[0]
                        + r_ref[s, t, 3 * r + 1 : 3 * r + 2, at] * pos[1]
                        + r_ref[s, t, 3 * r + 2 : 3 * r + 3, at] * pos[2]
                        + center
                    )


def spread_kernel(*refs, n_img, k_modes):
    pk = refs[:n_img][::-1]
    z_ref, r_ref, c_ref = refs[n_img:]
    lanes = z_ref.shape[3]
    for s in range(STEPS):
        for t in range(n_img):
            z_ref[s, t] = jnp.broadcast_to(pk[t][0:k_modes, s : s + 1], (k_modes, lanes))
            r_ref[s, t] = jnp.broadcast_to(pk[t][k_modes : k_modes + 8, s : s + 1], (8, lanes))
    for s in range(STEPS - 1):
        for t in range(n_img):
            zz = jnp.sum(z_ref[s + 1, 0] * z_ref[s, t], axis=0, keepdims=True)
            for r in range(2):
                for r2 in range(2):
                    d = None
                    for c in range(3):
                        e = (
                            r_ref[s + 1, 0, 3 * r + c : 3 * r + c + 1]
                            * r_ref[s, t, 3 * r2 + c : 3 * r2 + c + 1]
                        )
                        d = e if d is None else d + e
                    i = 2 * r + r2
                    c_ref[s, t, i : i + 1] = zz * d


def step_length(s_refs, entries):
    total = s_refs[0][...]
    for ref in s_refs[1:]:
        total = total + ref[...]
    total = jnp.sum(jnp.sum(total, axis=0, keepdims=True), axis=1, keepdims=True)
    return step_size / jnp.sqrt(total / entries + tiny_eps)


def forward_kernel(*refs, n_img, outer, entries, rows, nz):
    p_refs = refs[:n_img][::-1]
    pos = n_img
    if outer:
        q_ref = refs[pos]
        s_refs = refs[pos + 1 : pos + 1 + nz]
        pos += 1 + nz
    par_ref, obs_ref, keep_ref, send_ref, proj_ref, u_ref, v_ref, acc_ref, pix_ref = refs[pos:]
    pix, lanes = pix_ref.shape
    place = lax.axis_index("gauss")
    core = place % 2
    if outer:
        alpha = step_length(s_refs, entries)
    for t in range(n_img):
        p = p_refs[t][outer]
        if outer:
            p = p - alpha * q_ref[t]
        proj_ref[t] = p
    pix_ref[...] = lax.broadcasted_iota(jnp.int32, (pix, lanes), 0).astype(jnp.float32)
    acc_ref[...] = jnp.zeros_like(acc_ref)

    def slot(t, carry):
        total = None
        for j in range(SUB):
            c = par_ref[t, 0, j : j + 1, :]
            a = par_ref[t, 1, j : j + 1, :]
            du = pix_ref[...] - proj_ref[t, 0, j : j + 1, :]
            dv = pix_ref[...] - proj_ref[t, 1, j : j + 1, :]
            u = jnp.exp2(du * du * c).astype(jnp.bfloat16)
            v = (a * jnp.exp2(dv * dv * c)).astype(jnp.bfloat16)
            u_ref[t, j] = u
            v_ref[t, j] = v
            term = lax.dot_general(
                u, v, (((1,), (1,)), ((), ())), preferred_element_type=jnp.float32
            )
            total = term if total is None else total + term
        acc_ref[...] += total
        return carry

    lax.fori_loop(0, n_img, slot, 0)
    for z in range(nz):
        keep_ref[z] = acc_ref[pl.ds(pl.multiple_of((2 * z + core) * rows, 8), rows), :]
        send_ref[z] = acc_ref[pl.ds(pl.multiple_of((2 * z + 1 - core) * rows, 8), rows), :]
    keep_ref[place // 2] -= obs_ref[outer]


def moment(profile, weighted, mean):
    pix, lanes = weighted.shape
    n = pix // SUB
    run = None
    runs = None
    for i in range(n):
        x = profile[SUB * i : SUB * (i + 1)].astype(jnp.float32) * weighted[SUB * i : SUB * (i + 1)]
        run = x if run is None else run + x
        if i + 1 < n:
            runs = run if runs is None else runs + run
    sub = lax.broadcasted_iota(jnp.int32, (SUB, lanes), 0).astype(jnp.float32)
    at = sub - mean + float(SUB * (n - 1))
    return jnp.sum(run * at - float(SUB) * runs, axis=0, keepdims=True)


def backward_kernel(
    own_ref, other_ref, proj_ref, par_ref, u_ref, v_ref, out_ref, res_ref, rest_ref,
    *, n_img, rows, nz
):
    core = lax.axis_index("gauss") % 2
    for z in range(nz):
        res_ref[pl.ds(pl.multiple_of((2 * z + core) * rows, 16), rows), :] = own_ref[z]
        res_ref[pl.ds(pl.multiple_of((2 * z + 1 - core) * rows, 16), rows), :] = other_ref[z]
    rest_ref[...] = res_ref[...].astype(jnp.float32).T.astype(jnp.bfloat16)

    def slot(t, carry):
        for j in range(SUB):
            inv = par_ref[t, 2, j : j + 1, :]
            u = u_ref[t, j]
            v = v_ref[t, j]
            wu = jnp.dot(res_ref[...], v, preferred_element_type=jnp.float32)
            wv = jnp.dot(rest_ref[...], u, preferred_element_type=jnp.float32)
            mu = proj_ref[t, 0, j : j + 1, :]
            mv = proj_ref[t, 1, j : j + 1, :]
            out_ref[t, 0, j : j + 1, :] = inv * moment(u, wu, mu)
            out_ref[t, 1, j : j + 1, :] = inv * moment(v, wv, mv)
        return carry

    lax.fori_loop(0, n_img, slot, 0, unroll=4)


def shifts_of(r_ref, s, t, gu, gv, c):
    return r_ref[s, t, c : c + 1] * gu + r_ref[s, t, 3 + c : 4 + c] * gv


def squares_kernel(*refs, n_img, outer, with_q):
    z_ref, r_ref, c_ref = refs[:3]
    g = refs[3 : 3 + n_img][::-1]
    outs = refs[3 + n_img :]
    s_ref, shift_ref = outs[0], outs[-1]
    k_modes, lanes = z_ref.shape[2:]
    z = [z_ref[outer, t] for t in range(n_img)]
    squares = jnp.zeros((k_modes, lanes), jnp.float32)
    for t0 in range(n_img):
        gu = [g[t][t0 ^ t, 0].astype(jnp.float32) for t in range(n_img)]
        gv = [g[t][t0 ^ t, 1].astype(jnp.float32) for t in range(n_img)]
        for r in range(2 if with_q else 0):
            q = None
            for t in range(n_img):
                e = (
                    c_ref[outer, t, 2 * r : 2 * r + 1] * gu[t]
                    + c_ref[outer, t, 2 * r + 1 : 2 * r + 2] * gv[t]
                )
                q = e if q is None else q + e
            outs[1][t0, r] = q
        for c in range(3):
            for t in range(n_img):
                shift_ref[t0, c, t] = shifts_of(r_ref, outer, t, gu[t], gv[t], c)
    for t0 in range(n_img):
        for c in range(3):
            for j in range(SUB):
                m = None
                for t in range(n_img):
                    e = z[t] * shift_ref[t0, c, t, j : j + 1]
                    m = e if m is None else m + e
                squares = squares + m * m
    part = None
    for k in range(0, k_modes, SUB):
        for i in range(0, lanes, 128):
            e = squares[k : k + SUB, i : i + 128]
            part = e if part is None else part + e
    s_ref[...] = part


def update_kernel(*refs, n_img, nz, entries):
    z_ref, r_ref = refs[:2]
    pos = 2
    g = [refs[pos + s * n_img : pos + (s + 1) * n_img][::-1] for s in range(STEPS)]
    pos += STEPS * n_img
    s_refs = [refs[pos + s * nz : pos + (s + 1) * nz] for s in range(STEPS)]
    modes_ref, out_hbm, out_ref, shift_ref, sem = refs[pos + STEPS * nz :]
    lanes = z_ref.shape[3]
    for s in range(STEPS):
        alpha = step_length(s_refs[s], entries)
        for t in range(n_img):
            gu = alpha * g[s][t][t, 0].astype(jnp.float32)
            gv = alpha * g[s][t][t, 1].astype(jnp.float32)
            for c in range(3):
                shift_ref[s, t, c] = shifts_of(r_ref, s, t, gu, gv, c)
    for c in range(3):
        for j in range(SUB):
            m = modes_ref[c, :, j * lanes : (j + 1) * lanes]
            for s in range(STEPS):
                for t in range(n_img):
                    m = m - z_ref[s, t] * shift_ref[s, t, c, j : j + 1]
            out_ref[c, :, j * lanes : (j + 1) * lanes] = m
        pltpu.make_async_copy(out_ref.at[c], out_hbm.at[c], sem.at[c]).start()
    for c in range(3):
        pltpu.make_async_copy(out_ref.at[c], out_hbm.at[c], sem.at[c]).wait()


def body(
    observed, pose_index, batch_order, latents, base_positions, amplitudes, widths, deform_modes
):
    n_img = lax.axis_size("img")
    n_gauss = lax.axis_size("gauss")
    zplace = lax.axis_index("gauss") // 2
    nz = n_gauss // 2
    _, rows, pix = observed.shape
    k_modes, _, own = deform_modes.shape
    entries = 3 * k_modes * base_positions.shape[1] * n_gauss
    lanes = own // SUB
    modes = jnp.transpose(deform_modes, (1, 0, 2))
    part_fn = functools.partial

    pack = call(
        pack_kernel, "pack", f32(k_modes + 8, 128), (batch_order, pose_index, latents), [HBM] * 3,
        [pltpu.SMEM(batch_order.shape, jnp.int32), pltpu.SMEM(pose_index.shape, jnp.int32),
         pltpu.VMEM(latents.shape, jnp.float32), pltpu.SemaphoreType.DMA((3,))],
        pltpu.CompilerParams(vmem_limit_bytes=67018752),
    )
    pk = spread_out([pack] * n_img, "img")
    own_base, modes, dense_base, dense = call(
        own_kernel, "own",
        [f32(3, own), f32(3, k_modes, own), f32(3, SUB, lanes),
         f32(3, lanes // 128, k_modes * SUB, 128)],
        (base_positions, modes), [HBM] * 2, [pltpu.SemaphoreType.DMA((2,))],
    )
    par, obs = call(
        prepare_kernel, "prepare", [f32(n_img, 3, SUB, lanes), f32(STEPS, rows, pix)],
        (pack, observed, amplitudes, widths),
    )
    zs, rs, cs = call(
        part_fn(spread_kernel, n_img=n_img, k_modes=k_modes), "spread",
        [f32(STEPS, n_img, k_modes, lanes), f32(STEPS, n_img, 8, lanes),
         f32(STEPS - 1, n_img, 8, lanes)],
        pk[::-1],
    )
    proj = call(
        part_fn(project_kernel, center=(pix - 1) * 0.5), "project",
        [f32(STEPS, 2, SUB, lanes)] * n_img, (zs, rs, dense_base, dense),
    )[::-1]
    proj = spread_out(proj, "img")

    extra = []
    grads, sums = [], []
    half_shape = f32(nz, rows, pix)
    per_shard = f32(n_img, 2, SUB, lanes)
    profile = jax.ShapeDtypeStruct((n_img, SUB, pix, lanes), jnp.bfloat16)
    for outer in range(STEPS):
        keep, send, here, u, v = call(
            part_fn(forward_kernel, n_img=n_img, outer=outer, entries=entries, rows=rows, nz=nz),
            "forward", [half_shape, half_shape, per_shard, profile, profile], (*proj[::-1], *extra, par, obs),
            scratch=[pltpu.VMEM((pix, pix), jnp.float32), pltpu.VMEM((pix, lanes), jnp.float32)],
        )
        part = keep + exchange(send, "gauss", 1)
        bit = 2
        while bit < n_gauss:
            part = part + exchange(part.astype(jnp.bfloat16), "gauss", bit).astype(jnp.float32)
            bit *= 2
        half = part.astype(jnp.bfloat16)
        other = exchange(half, "gauss", 1)
        g = call(
            part_fn(backward_kernel, n_img=n_img, rows=rows, nz=nz), "backward", per_shard,
            (half, other, here, par, u, v),
            scratch=[pltpu.VMEM((pix, pix), jnp.bfloat16)] * 2,
        )
        g = spread_out([g] + [g.astype(jnp.bfloat16)] * (n_img - 1), "img")
        more = outer + 1 < STEPS
        out = call(
            part_fn(squares_kernel, n_img=n_img, outer=outer, with_q=more), "squares",
            [f32(SUB, 128)] + [per_shard] * more, (zs, rs, cs, *g[::-1]),
            scratch=[pltpu.VMEM((n_img, 3, n_img, SUB, lanes), jnp.float32)],
        )
        s_chip = out[0] + exchange(out[0], "gauss", 1)
        s_all = spread_out([s_chip] * nz, "gauss", 2)
        extra = [out[-1], *s_all[::-1]]
        grads.extend(g[::-1])
        sums.extend(s_all[::-1])
    final_rows = lax.dynamic_index_in_dim(part, zplace, 0, keepdims=False)
    new = pl.pallas_call(
        part_fn(update_kernel, n_img=n_img, nz=nz, entries=entries),
        out_shape=f32(*modes.shape),
        in_specs=[VMEM] * (3 + STEPS * (n_img + nz)),
        out_specs=HBM,
        scratch_shapes=[
            pltpu.VMEM(modes.shape, jnp.float32),
            pltpu.VMEM((STEPS, n_img, 3, SUB, lanes), jnp.float32),
            pltpu.SemaphoreType.DMA((3,)),
        ],
        compiler_params=PARAMS,
        name="update",
    )(zs, rs, *grads, *sums, modes)
    return (final_rows[None], jnp.transpose(new, (1, 0, 2)))


def solution(mesh):
    return jax.shard_map(
        body,
        mesh=mesh,
        in_specs=(
            P("img", "gauss", None),
            P("img"),
            P("img"),
            P("img", None),
            P(None, "gauss"),
            P("gauss"),
            P("gauss"),
            P(None, None, ("gauss", "img")),
        ),
        out_specs=(P("img", "gauss", None), P(None, None, ("gauss", "img"))),
        check_vma=False,
    )
```
